128 devices in a mesh: tasks: 1, col: 2 (over core), row: 64 (over z, y, x).
Axes of the slice: x: 4, y: 4, z: 4, core: 2. Of those that a mesh axis runs over, the one named last changes fastest.
Arguments:
- x_pts: bfloat16 [98304, 128], P(('tasks', 'row', 'col'))
- v_rhs: bfloat16 [98304, 32], P(('tasks', 'row', 'col'))
- length_scale: float32 [1], replicated
- out_scale: float32 [1], replicated
Outputs:
- output: float32 [98304, 32], P(('tasks', 'row', 'col'))
All inputs are finite; a program needn't handle non-finite values.
Results may differ from the reference program's by a relative error of at most 0.001.
Values are sent between devices in bfloat16 or wider.
A program may use at most 1 GiB of HBM per device.

```python
import jax
import jax.numpy as jnp
from jax import lax

ROWS_DEV = 768
GROUP = 64
COLS = 2
FEAT = 128
RHS = 32
CLUSTERS = 16
N_PTS = ROWS_DEV * GROUP * COLS
TILE_ROWS = ROWS_DEV


def setup_inputs(seed: int = 0, part: int = 0) -> dict:
    part_key = jax.random.fold_in(jax.random.key(seed), part)
    k_cent, k_assign, k_noise, k_mean, k_vals = jax.random.split(part_key, 5)
    k_len, k_out = jax.random.split(jax.random.key(seed + 1), 2)
    centers = jax.random.normal(k_cent, (CLUSTERS, FEAT), jnp.float32)
    assign = jax.random.randint(k_assign, (N_PTS,), 0, CLUSTERS)
    pt_noise = jax.random.normal(k_noise, (N_PTS, FEAT), jnp.float32)
    x_pts = (centers[assign] + 0.7 * pt_noise).astype(jnp.bfloat16)
    col_mean = jax.random.uniform(k_mean, (1, RHS), jnp.float32, -1.5, 1.5) * N_PTS ** -0.5
    v_vals = jax.random.normal(k_vals, (N_PTS, RHS), jnp.float32)
    v_rhs = (col_mean + v_vals).astype(jnp.bfloat16)
    len_draw = jax.random.uniform(k_len, (1,), jnp.float32, 0.75, 1.25)
    length_scale = jnp.sqrt(1.5 * FEAT * len_draw)
    out_scale = jax.random.uniform(k_out, (1,), jnp.float32, 0.5, 1.5) * N_PTS ** -0.5
    return {"x_pts": x_pts, "v_rhs": v_rhs, "length_scale": length_scale, "out_scale": out_scale}


def reference(x_pts, v_rhs, length_scale, out_scale):
    two_ell_sq = 2.0 * length_scale[0] * length_scale[0]
    sq_norms = jnp.sum(jnp.square(x_pts.astype(jnp.float32)), axis=1)
    n_tiles = N_PTS // TILE_ROWS
    x_tiles = x_pts.reshape(n_tiles, TILE_ROWS, FEAT)
    norm_tiles = sq_norms.reshape(n_tiles, TILE_ROWS)
    v_tiles = v_rhs.reshape(n_tiles, TILE_ROWS, RHS)

    def target_rows(tgt_pair):
        x_tgt, n_tgt = tgt_pair

        def src_step(acc_rows, src_triple):
            x_src, n_src, v_src = src_triple
            gram_mat = jnp.dot(x_tgt, x_src.T, preferred_element_type=jnp.float32)
            sq_dist = jnp.maximum(n_tgt[:, None] + n_src[None, :] - 2.0 * gram_mat, 0.0)
            kern_bf = (out_scale[0] * jnp.exp(-sq_dist / two_ell_sq)).astype(jnp.bfloat16)
            return acc_rows + jnp.dot(kern_bf, v_src, preferred_element_type=jnp.float32), None

        acc_rows, _ = lax.scan(src_step, jnp.zeros((TILE_ROWS, RHS), jnp.float32), (x_tiles, norm_tiles, v_tiles))
        return acc_rows

    y_tiles = lax.map(target_rows, (x_tiles, norm_tiles))
    return y_tiles.reshape(N_PTS, RHS)
```

```python
import functools

import jax
import jax.numpy as jnp
from jax import lax
from jax.experimental import pallas as pl
from jax.experimental.pallas import tpu as pltpu
from jax.sharding import PartitionSpec as P

BF = jnp.bfloat16
F32 = jnp.float32
ROWS = 768
FEAT = 128
RHS = 32
NSRC = 32
NTGT = 4
GROUPS = 6
VROWS = GROUPS * RHS
SROWS = ROWS + VROWS
XROWS = 144
TILES = 3
STEPS = 24
PAIRS = 6
TRIPS = NSRC * TILES // STEPS
LOG2E = 1.4426950408889634
BIG = 3.0e38


def pieces(norm):
    half = jnp.maximum(norm * -0.5, -BIG)
    hi = half.astype(BF).astype(F32)
    rest = half - hi
    mid = rest.astype(BF).astype(F32)
    return hi, mid, rest - mid


def select(pos, at, vals):
    out = jnp.zeros_like(vals[0] + pos.astype(F32))
    for k, val in enumerate(vals):
        out = jnp.where(pos == at + k, val, out)
    return out


def position():
    col = lax.axis_index("col")
    row = lax.axis_index("row")
    return col, row // 16, (row // 4) % 4, row % 4


def device(col, z, y, x):
    return (0, col, (z % 4) * 16 + (y % 4) * 4 + x % 4)


def enter(peers):
    barrier = pltpu.get_barrier_semaphore()
    for peer in peers:
        pl.semaphore_signal(barrier, inc=1, device_id=peer, device_id_type=pl.DeviceIdType.MESH)
    pl.semaphore_wait(barrier, len(peers))


def gather_kernel(x_ref, v_ref, sx_ref, aug_ref, xt_ref, ssem, rsem, tsend, trecv):
    c, z, y, x = position()
    partner = device(1 - c, z, y, x)

    sx_ref[0, 0:ROWS, :] = x_ref[...]
    for g in range(GROUPS):
        sx_ref[0, ROWS + g * RHS : ROWS + (g + 1) * RHS, :] = v_ref[:, g * 128 : (g + 1) * 128]
    xt = jnp.transpose(x_ref[...].astype(F32))
    nrm = jnp.sum(xt * xt, axis=0, keepdims=True)
    hi, mid, low = pieces(nrm)
    pos = lax.broadcasted_iota(jnp.int32, (16, 128), 0)
    for g in range(GROUPS):
        s = slice(g * 128, (g + 1) * 128)
        xt_ref[0, g, 0:FEAT, :] = xt[:, s].astype(BF)
        one = jnp.ones((1, 128), F32)
        xt_ref[0, g, FEAT:XROWS, :] = select(pos, 0, (hi[:, s], mid[:, s], low[:, s], one, one, one)).astype(BF)

    enter([partner, device(c, z + 1, y, x), device(c, z + 3, y, x), device(c, z, y + 1, x),
           device(c, z, y + 3, x), device(c, z, y, x + 1), device(c, z, y, x + 3)])

    copies = []

    def send(src, dst, dev):
        cp = pltpu.make_async_remote_copy(sx_ref.at[src], sx_ref.at[dst], ssem.at[len(copies)], rsem.at[dst],
                                          device_id=dev, device_id_type=pl.DeviceIdType.MESH)
        cp.start()
        copies.append(cp)

    def got(slot):
        pltpu.make_async_remote_copy(sx_ref.at[slot], sx_ref.at[slot], ssem.at[0], rsem.at[slot],
                                     device_id=partner, device_id_type=pl.DeviceIdType.MESH).wait_recv()

    tcopies = []

    def tsnd(src, dst, dev):
        cp = pltpu.make_async_remote_copy(xt_ref.at[src, :, pl.ds(0, XROWS), :], xt_ref.at[dst, :, pl.ds(0, XROWS), :],
                                          tsend.at[len(tcopies)], trecv.at[dst],
                                          device_id=dev, device_id_type=pl.DeviceIdType.MESH)
        cp.start()
        tcopies.append(cp)

    def tgot(slot):
        pltpu.make_async_remote_copy(xt_ref.at[slot, :, pl.ds(0, XROWS), :], xt_ref.at[slot, :, pl.ds(0, XROWS), :],
                                     tsend.at[0], trecv.at[slot],
                                     device_id=partner, device_id_type=pl.DeviceIdType.MESH).wait_recv()

    def pos_slot(dz, dy):
        return (dz * 4 + dy) * 2

    lane = lax.broadcasted_iota(jnp.int32, (128, 128), 1)

    def build(slot):
        def chunk(i, carry):
            rows = pl.ds(pl.multiple_of(i * 128, 128), 128)
            xs = sx_ref[slot, rows, :].astype(F32)
            nj = jnp.sum(xs * xs, axis=1, keepdims=True)
            hi, mid, low = pieces(nj)
            one = jnp.ones((128, 1), F32)
            aug_ref[slot, rows, :] = select(lane, 0, (one, one, one, hi, mid, low)).astype(BF)
            return carry

        lax.fori_loop(0, ROWS // 128, chunk, 0)

    sgn = 1 - 2 * c
    send(pos_slot(0, 0), pos_slot(3, 0), device(c, z + 1, y, x))
    send(pos_slot(0, 0), pos_slot(1, 0), device(c, z + 3, y, x))
    send(pos_slot(0, 0), pos_slot(0, 3), device(c, z, y + 1, x))
    send(pos_slot(0, 0), pos_slot(0, 1), device(c, z, y + 3, x))
    tsnd(0, 3, device(c, z, y, x + 1))
    tsnd(0, 1, device(c, z, y, x + 3))
    send(pos_slot(0, 0), 1, partner)
    for t in range(NTGT):
        for g in range(GROUPS):
            xt_ref[t, g, XROWS:256, :] = jnp.zeros((256 - XROWS, 128), BF)
    build(0)
    got(1)
    build(1)

    near = 2 + sgn
    far = 2 - sgn
    got(pos_slot(near, 0))
    send(pos_slot(near, 0), pos_slot(2, 0), device(c, z + sgn, y, x))
    got(pos_slot(0, near))
    send(pos_slot(0, near), pos_slot(0, 2), device(c, z, y + sgn, x))
    tgot(2 + sgn)
    tsnd(2 + sgn, 2, device(c, z, y, x + sgn))
    got(pos_slot(far, 0))
    got(pos_slot(0, far))

    def cross(k, m):
        return (k * (4 - 3 * c) + m * (1 + 3 * c)) * 2

    def ahead(d):
        return device(c, z + d * c, y + d * (1 - c), x)

    def pass_on(k):
        send(cross(k, 0), cross(k, 3), ahead(1))
        send(cross(k, 0), cross(k, 1), ahead(3))

    def share(slot):
        send(slot, slot + 1, partner)

    pass_on(1)
    pass_on(3)
    for s in (pos_slot(1, 0), pos_slot(3, 0), pos_slot(0, 1), pos_slot(0, 3)):
        share(s)
        build(s)
    got(pos_slot(2, 0))
    got(pos_slot(0, 2))
    pass_on(2)
    for s in (pos_slot(2, 0), pos_slot(0, 2)):
        share(s)
        build(s)
    for s in (pos_slot(1, 0), pos_slot(3, 0), pos_slot(0, 1), pos_slot(0, 3), pos_slot(2, 0), pos_slot(0, 2)):
        got(s + 1)
        build(s + 1)
    for k, d in ((1, 1), (3, 3), (2, 1)):
        a = 2 + d if d == 1 else 1
        b = 4 - a
        got(cross(k, a))
        send(cross(k, a), cross(k, 2), ahead(d))
        share(cross(k, a))
        build(cross(k, a))
        got(cross(k, b))
        share(cross(k, b))
        build(cross(k, b))
    for k in (1, 3, 2):
        got(cross(k, 2))
        share(cross(k, 2))
        build(cross(k, 2))
    for k in (1, 3, 2):
        for m in (1, 3, 2):
            got(pos_slot(k, m) + 1)
            build(pos_slot(k, m) + 1)
    tgot(2 - sgn)
    tgot(2)
    for cp in copies:
        cp.wait_send()
    for cp in tcopies:
        cp.wait_send()


def product_kernel(sc_ref, sx_ref, aug_ref, xt_ref, y_ref, tile_ref):
    alpha = sc_ref[0]
    scale = sc_ref[1]
    piece = 64
    n_pc = 256 // piece

    def run(*accs):
        per = 3 * n_pc + 2
        gram = [[[accs[q * per + r * n_pc + p] for p in range(n_pc)] for r in range(3)] for q in range(2)]
        body_acc = [accs[q * per + 3 * n_pc] for q in range(2)]
        tail_acc = [accs[q * per + 3 * n_pc + 1] for q in range(2)]

        def acc_gram(q, u, blk, tile, p):
            rows = pl.ds(tile * 256 + p * piece, piece)
            lhs = jnp.concatenate([sx_ref[blk, rows, :], aug_ref[blk, rows, :]], axis=1)
            pltpu.matmul_acc_lhs(gram[q][u % 3][p], lhs, load_staged_rhs=0 if p == 0 else None)

        def push_x(q, pair):
            tgt = (pair // 3) * 2 + q
            ch = (pair % 3) * 2
            pltpu.matmul_push_rhs(jnp.concatenate([xt_ref[tgt, ch], xt_ref[tgt, ch + 1]], axis=1),
                                  staging_register=0, mxu_index=q)

        def push_tile(q, u):
            pltpu.matmul_push_rhs(tile_ref[q, (u - 1) % 2], staging_register=1, mxu_index=q)

        def values(q, u, p):
            half = pltpu.matmul_pop(gram[q][(u - 2) % 3][p])
            kern = (jnp.exp2(jnp.minimum(half * alpha, 0.0)) * scale).astype(BF)
            tile_ref[q, u % 2, p * piece : (p + 1) * piece, :] = kern

        def acc_y(q, u, blk, tile, acc):
            lo = ROWS + tile * 2 * RHS
            vt = jnp.concatenate([sx_ref[blk, lo : lo + RHS, :], sx_ref[blk, lo + RHS : lo + 2 * RHS, :]], axis=1)
            pltpu.matmul_acc_lhs(acc[q], vt, load_staged_rhs=1)

        def add_y(acc, pair):
            for q in range(2):
                y_ref[(pair // 3) * 2 + q, pair % 3] += pltpu.matmul_pop(acc[q])

        def trip(k, carry):
            pair = k // TRIPS
            blk0 = (k % TRIPS) * (STEPS // TILES)
            last = k + TRIPS * PAIRS - 1
            old_blk0 = (last % TRIPS) * (STEPS // TILES)
            old_pair = jnp.where(k == 0, PAIRS, (k - 1) // TRIPS)
            for u in range(STEPS):
                blk, tile = blk0 + u // TILES, u % TILES
                nxt = pair if u < STEPS - 1 else jnp.minimum((k + 1) // TRIPS, PAIRS - 1)
                for q in range(2):
                    push_tile(q, u)
                for p in range(n_pc):
                    for q in range(2):
                        acc_gram(q, u, blk, tile, p)
                        if p == 0:
                            push_x(q, nxt)
                    for q in range(2):
                        values(q, u, p)
                for q in range(2):
                    if u < 3:
                        w = STEPS - 3 + u
                        acc_y(q, u, old_blk0 + w // TILES, w % TILES, tail_acc)
                    else:
                        w = u - 3
                        acc_y(q, u, blk0 + w // TILES, w % TILES, body_acc)
                if u == 1:
                    add_y(body_acc, old_pair)
                if u == 6:
                    add_y(tail_acc, old_pair)
            return carry

        for q in range(2):
            for r in range(3):
                for p in range(n_pc):
                    pltpu.matmul_pop(gram[q][r][p])
            pltpu.matmul_pop(body_acc[q])
            pltpu.matmul_pop(tail_acc[q])
            push_x(q, 0)
        y_ref[...] = jnp.zeros_like(y_ref)
        lax.fori_loop(0, TRIPS * PAIRS, trip, 0)
        for u in range(STEPS, STEPS + 3):
            w = u - 3
            for q in range(2):
                push_tile(q, u)
                if u < STEPS + 2:
                    for p in range(n_pc):
                        values(q, u, p)
                acc_y(q, u, NSRC - STEPS // TILES + w // TILES, w % TILES, tail_acc)
        add_y(body_acc, PAIRS - 1)
        for q in range(2):
            acc_gram(q, 0, 0, 0, 0)
            pltpu.matmul_pop(gram[q][0][0])
        add_y(tail_acc, PAIRS - 1)

    specs = []
    for q in range(2):
        specs += [pltpu.ACC(q)((piece, 256), F32)] * (3 * n_pc) + [pltpu.ACC(q)((RHS, 256), F32)] * 2
    pl.run_scoped(run, *specs)


def reduce_kernel(yp_ref, y_ref, got_ref, ssem, rsem):
    c, z, y, x = position()
    enter([device(c, z, y, x + d) for d in (1, 2, 3)])
    copies = []
    for d in (2, 1, 3):
        cp = pltpu.make_async_remote_copy(yp_ref.at[d], got_ref.at[d - 1], ssem.at[d - 1], rsem.at[d - 1],
                                          device_id=device(c, z, y, x + d), device_id_type=pl.DeviceIdType.MESH)
        cp.start()
        copies.append(cp)
    for cp in copies:
        cp.wait()
    for ch in range(3):
        tot = yp_ref[0, ch] + got_ref[0, ch] + got_ref[1, ch] + got_ref[2, ch]
        y_ref[:, ch * 256 : (ch + 1) * 256] = tot


VM = pl.BlockSpec(memory_space=pltpu.VMEM)
SM = pl.BlockSpec(memory_space=pltpu.SMEM)


def solution(mesh):
    def local_rows(x_loc, v_loc, length_scale, out_scale):
        two_ell_sq = 2.0 * length_scale[0] * length_scale[0]
        consts = jnp.stack([(2.0 * LOG2E) / two_ell_sq, out_scale[0]])
        sx, aug, xt = pl.pallas_call(
            gather_kernel,
            out_shape=(jax.ShapeDtypeStruct((NSRC, SROWS, 128), BF), jax.ShapeDtypeStruct((NSRC, ROWS, 128), BF),
                       jax.ShapeDtypeStruct((NTGT, GROUPS, 256, 128), BF)),
            in_specs=[VM, VM],
            out_specs=(VM, VM, VM),
            scratch_shapes=[pltpu.SemaphoreType.DMA((40,)), pltpu.SemaphoreType.DMA((NSRC,)),
                            pltpu.SemaphoreType.DMA((4,)), pltpu.SemaphoreType.DMA((NTGT,))],
            compiler_params=pltpu.CompilerParams(collective_id=0, has_side_effects=True, vmem_limit_bytes=24 * 2**20),
            name="gather",
        )(x_loc, v_loc.T)
        yp = pl.pallas_call(
            product_kernel,
            out_shape=jax.ShapeDtypeStruct((6, 3, RHS, 256), F32),
            in_specs=[SM, VM, VM, VM],
            out_specs=VM,
            scratch_shapes=[pltpu.VMEM((2, 2, 256, 256), BF)],
            compiler_params=pltpu.CompilerParams(vmem_limit_bytes=24 * 2**20),
            name="product",
        )(consts, sx, aug, xt)
        y_t = pl.pallas_call(
            reduce_kernel,
            out_shape=jax.ShapeDtypeStruct((RHS, ROWS), F32),
            in_specs=[VM],
            out_specs=VM,
            scratch_shapes=[pltpu.VMEM((3, 3, RHS, 256), F32), pltpu.SemaphoreType.DMA((3,)), pltpu.SemaphoreType.DMA((3,))],
            compiler_params=pltpu.CompilerParams(collective_id=1, has_side_effects=True, vmem_limit_bytes=8 * 2**20),
            name="reduce",
        )(yp)
        return y_t.T

    row_spec = P(("tasks", "row", "col"), None)
    rep_spec = P(None)
    return jax.shard_map(local_rows, mesh=mesh, in_specs=(row_spec, row_spec, rep_spec, rep_spec), out_specs=row_spec, check_vma=False)
```

```python
import functools

import jax
import jax.numpy as jnp
from jax import lax
from jax.experimental import pallas as pl
from jax.experimental.pallas import tpu as pltpu
from jax.sharding import PartitionSpec as P

BF = jnp.bfloat16
F32 = jnp.float32
ROWS = 768
FEAT = 128
RHS = 32
NEAR = 7
NTGT = 8
GROUPS = 6
VROWS = GROUPS * RHS
SROWS = ROWS + VROWS
XROWS = 144
TILES = 3
PAIRS = 12
LOG2E = 1.4426950408889634
BIG = 3.0e38


def pieces(norm):
    half = jnp.maximum(norm * -0.5, -BIG)
    hi = half.astype(BF).astype(F32)
    rest = half - hi
    mid = rest.astype(BF).astype(F32)
    return hi, mid, rest - mid


def select(pos, at, vals):
    out = jnp.zeros_like(vals[0] + pos.astype(F32))
    for k, val in enumerate(vals):
        out = jnp.where(pos == at + k, val, out)
    return out


def position():
    col = lax.axis_index("col")
    row = lax.axis_index("row")
    return col, row // 16, (row // 4) % 4, row % 4


def device(col, z, y, x):
    return (0, col, (z % 4) * 16 + (y % 4) * 4 + x % 4)


def enter(peers):
    barrier = pltpu.get_barrier_semaphore()
    for peer in peers:
        pl.semaphore_signal(barrier, inc=1, device_id=peer, device_id_type=pl.DeviceIdType.MESH)
    pl.semaphore_wait(barrier, len(peers))


def build_aug(src, dst):
    lane = lax.broadcasted_iota(jnp.int32, (128, 128), 1)

    def chunk(i, carry):
        rows = pl.ds(pl.multiple_of(i * 128, 128), 128)
        xs = src[rows, :].astype(F32)
        nj = jnp.sum(xs * xs, axis=1, keepdims=True)
        hi, mid, low = pieces(nj)
        one = jnp.ones((128, 1), F32)
        dst[rows, :] = select(lane, 0, (one, one, one, hi, mid, low)).astype(BF)
        return carry

    lax.fori_loop(0, ROWS // 128, chunk, 0)


def gather_kernel(x_ref, v_ref, sx_ref, aug_ref, xt_ref, ssem, rsem, tsend, trecv):
    c, z, y, x = position()
    partner = device(1 - c, z, y, x)

    sx_ref[0, 0:ROWS, :] = x_ref[...]
    for g in range(GROUPS):
        sx_ref[0, ROWS + g * RHS : ROWS + (g + 1) * RHS, :] = v_ref[:, g * 128 : (g + 1) * 128]
    xt = jnp.transpose(x_ref[...].astype(F32))
    nrm = jnp.sum(xt * xt, axis=0, keepdims=True)
    hi, mid, low = pieces(nrm)
    pos = lax.broadcasted_iota(jnp.int32, (16, 128), 0)
    for g in range(GROUPS):
        s = slice(g * 128, (g + 1) * 128)
        xt_ref[0, g, 0:FEAT, :] = xt[:, s].astype(BF)
        one = jnp.ones((1, 128), F32)
        xt_ref[0, g, FEAT:XROWS, :] = select(pos, 0, (hi[:, s], mid[:, s], low[:, s], one, one, one)).astype(BF)

    enter([partner, device(c, z + 1, y, x), device(c, z + 3, y, x), device(c, z, y + 1, x),
           device(c, z, y + 3, x), device(c, z, y, x + 1), device(c, z, y, x + 3)])

    copies = []

    def send(src, dst, dev):
        cp = pltpu.make_async_remote_copy(sx_ref.at[src], sx_ref.at[dst], ssem.at[len(copies)], rsem.at[dst],
                                          device_id=dev, device_id_type=pl.DeviceIdType.MESH)
        cp.start()
        copies.append(cp)

    def got(slot):
        pltpu.make_async_remote_copy(sx_ref.at[slot], sx_ref.at[slot], ssem.at[0], rsem.at[slot],
                                     device_id=partner, device_id_type=pl.DeviceIdType.MESH).wait_recv()

    tcopies = []

    def tsnd(src, dst, dev):
        cp = pltpu.make_async_remote_copy(xt_ref.at[src, :, pl.ds(0, XROWS), :], xt_ref.at[dst, :, pl.ds(0, XROWS), :],
                                          tsend.at[len(tcopies)], trecv.at[dst],
                                          device_id=dev, device_id_type=pl.DeviceIdType.MESH)
        cp.start()
        tcopies.append(cp)

    def tgot(slot):
        pltpu.make_async_remote_copy(xt_ref.at[slot, :, pl.ds(0, XROWS), :], xt_ref.at[slot, :, pl.ds(0, XROWS), :],
                                     tsend.at[0], trecv.at[slot],
                                     device_id=partner, device_id_type=pl.DeviceIdType.MESH).wait_recv()

    zb = 3 * c
    yb = 3 - 3 * c
    sgn = 1 - 2 * c
    send(0, zb + 3, device(c, z + 1, y, x))
    send(0, zb + 1, device(c, z + 3, y, x))
    send(0, yb + 3, device(c, z, y + 1, x))
    send(0, yb + 1, device(c, z, y + 3, x))
    tsnd(0, 6, device(c, z, y, x + 1))
    tsnd(0, 2, device(c, z, y, x + 3))
    tsnd(0, 1, partner)
    for t in range(NTGT):
        for g in range(GROUPS):
            xt_ref[t, g, XROWS:256, :] = jnp.zeros((256 - XROWS, 128), BF)
    build_aug(sx_ref.at[0], aug_ref.at[0])

    near = 2 + sgn
    far = 2 - sgn
    tgot(2 * near)
    tsnd(2 * near, 4, device(c, z, y, x + sgn))
    tsnd(2 * near, 2 * near + 1, partner)
    got(zb + near)
    send(zb + near, zb + 2, device(c, z + sgn, y, x))
    got(yb + near)
    send(yb + near, yb + 2, device(c, z, y + sgn, x))
    tgot(2 * far)
    tsnd(2 * far, 2 * far + 1, partner)
    build_aug(sx_ref.at[zb + near], aug_ref.at[zb + near])
    build_aug(sx_ref.at[yb + near], aug_ref.at[yb + near])
    got(zb + far)
    build_aug(sx_ref.at[zb + far], aug_ref.at[zb + far])
    got(yb + far)
    build_aug(sx_ref.at[yb + far], aug_ref.at[yb + far])
    tgot(4)
    tsnd(4, 5, partner)
    got(zb + 2)
    build_aug(sx_ref.at[zb + 2], aug_ref.at[zb + 2])
    got(yb + 2)
    build_aug(sx_ref.at[yb + 2], aug_ref.at[yb + 2])
    for t in (1, 3, 5, 7):
        tgot(t)
    for cp in copies:
        cp.wait_send()
    for cp in tcopies:
        cp.wait_send()


def product(alpha, scale, blocks, xt_ref, y_ref, tile_ref):
    piece = 64
    n_pc = 256 // piece
    steps = len(blocks) * TILES

    def run(*accs):
        per = 3 * n_pc + 2
        gram = [[[accs[q * per + r * n_pc + p] for p in range(n_pc)] for r in range(3)] for q in range(2)]
        body_acc = [accs[q * per + 3 * n_pc] for q in range(2)]
        tail_acc = [accs[q * per + 3 * n_pc + 1] for q in range(2)]

        def acc_gram(q, u, t, p):
            sx, aug = blocks[t // TILES]
            rows = pl.ds((t % TILES) * 256 + p * piece, piece)
            lhs = jnp.concatenate([sx[rows, :], aug[rows, :]], axis=1)
            pltpu.matmul_acc_lhs(gram[q][u % 3][p], lhs, load_staged_rhs=0 if p == 0 else None)

        def push_x(q, pair):
            tgt = (pair // 3) * 2 + q
            ch = (pair % 3) * 2
            pltpu.matmul_push_rhs(jnp.concatenate([xt_ref[tgt, ch], xt_ref[tgt, ch + 1]], axis=1),
                                  staging_register=0, mxu_index=q)

        def push_tile(q, u):
            pltpu.matmul_push_rhs(tile_ref[q, (u - 1) % 3], staging_register=1, mxu_index=q)

        def values(q, u, p):
            half = pltpu.matmul_pop(gram[q][(u - 2) % 3][p])
            kern = (jnp.exp2(jnp.minimum(half * alpha, 0.0)) * scale).astype(BF)
            tile_ref[q, u % 3, p * piece : (p + 1) * piece, :] = kern

        def acc_y(q, t, acc):
            sx, _ = blocks[t // TILES]
            lo = ROWS + (t % TILES) * 2 * RHS
            vt = jnp.concatenate([sx[pl.ds(lo, RHS), :], sx[pl.ds(lo + RHS, RHS), :]], axis=1)
            pltpu.matmul_acc_lhs(acc[q], vt, load_staged_rhs=1)

        def add_y(acc, pair):
            for q in range(2):
                y_ref[q, pair // 3, pair % 3] += pltpu.matmul_pop(acc[q])

        def trip(k, carry):
            old = jnp.where(k == 0, PAIRS, k - 1)
            for u in range(steps):
                nxt = k if u < steps - 1 else jnp.minimum(k + 1, PAIRS - 1)
                for q in range(2):
                    push_tile(q, u)
                for p in range(n_pc):
                    for q in range(2):
                        acc_gram(q, u, u, p)
                        if p == 0:
                            push_x(q, nxt)
                    for q in range(2):
                        values(q, u, p)
                for q in range(2):
                    if u < 3:
                        acc_y(q, steps - 3 + u, tail_acc)
                    else:
                        acc_y(q, u - 3, body_acc)
                if u == 1:
                    add_y(body_acc, old)
                if u == 6:
                    add_y(tail_acc, old)
            return carry

        for q in range(2):
            for r in range(3):
                for p in range(n_pc):
                    pltpu.matmul_pop(gram[q][r][p])
            pltpu.matmul_pop(body_acc[q])
            pltpu.matmul_pop(tail_acc[q])
            push_x(q, 0)
        lax.fori_loop(0, PAIRS, trip, 0)
        for u in range(steps, steps + 3):
            for q in range(2):
                push_tile(q, u)
                if u < steps + 2:
                    for p in range(n_pc):
                        values(q, u, p)
                acc_y(q, u - 3, tail_acc)
        add_y(body_acc, PAIRS - 1)
        for q in range(2):
            acc_gram(q, 0, 0, 0)
            pltpu.matmul_pop(gram[q][0][0])
        add_y(tail_acc, PAIRS - 1)

    specs = []
    for q in range(2):
        specs += [pltpu.ACC(q)((piece, 256), F32)] * (3 * n_pc) + [pltpu.ACC(q)((RHS, 256), F32)] * 2
    pl.run_scoped(run, *specs)


def near_kernel(sc_ref, sx_ref, aug_ref, xt_ref, y_ref, tile_ref):
    y_ref[...] = jnp.zeros_like(y_ref)
    blocks = [(sx_ref.at[b], aug_ref.at[b]) for b in range(NEAR)]
    product(sc_ref[0], sc_ref[1], blocks, xt_ref, y_ref, tile_ref)


def far_kernel(sc_ref, s1_ref, s2_ref, s3_ref, xt_ref, yin_ref, y_ref, tile_ref, aug_ref):
    y_ref[...] = yin_ref[...]
    blocks = []
    for ref in (s1_ref, s2_ref, s3_ref):
        for b in range(3):
            blocks.append((ref.at[b], aug_ref.at[len(blocks)]))
    for sx, aug in blocks:
        build_aug(sx, aug)
    product(sc_ref[0], sc_ref[1], blocks, xt_ref, y_ref, tile_ref)


def reduce_kernel(yp_ref, y_ref, part_ref, stage_ref, got_ref, psend, precv, ssem, rsem):
    c, z, y, x = position()
    partner = device(1 - c, z, y, x)
    enter([partner] + [device(c, z, y, x + d) for d in (1, 2, 3)])
    order = (2, 1, 3, 0)
    first = []
    for d in order:
        cp = pltpu.make_async_remote_copy(yp_ref.at[1, d], part_ref.at[d], psend.at[d], precv.at[d],
                                          device_id=partner, device_id_type=pl.DeviceIdType.MESH)
        cp.start()
        first.append(cp)
    second = []
    for cp, d in zip(first, order):
        cp.wait()
        stage_ref[d] = yp_ref[0, d] + part_ref[d]
        if d:
            cp2 = pltpu.make_async_remote_copy(stage_ref.at[d], got_ref.at[d - 1], ssem.at[d - 1], rsem.at[d - 1],
                                               device_id=device(c, z, y, x + d), device_id_type=pl.DeviceIdType.MESH)
            cp2.start()
            second.append(cp2)
    for cp in second:
        cp.wait()
    for ch in range(3):
        y_ref[:, ch * 256 : (ch + 1) * 256] = stage_ref[0, ch] + got_ref[0, ch] + got_ref[1, ch] + got_ref[2, ch]


def cross_pairs(shift):
    pairs = []
    for c in range(2):
        for z in range(4):
            for y in range(4):
                for x in range(4):
                    z2 = (z + shift * c) % 4
                    y2 = (y + shift * (1 - c)) % 4
                    pairs.append((c * 64 + z * 16 + y * 4 + x, c * 64 + z2 * 16 + y2 * 4 + x))
    return pairs


VM = pl.BlockSpec(memory_space=pltpu.VMEM)
SM = pl.BlockSpec(memory_space=pltpu.SMEM)
FLOPS = 2 * ROWS * ROWS * (2 * FEAT + RHS) * NTGT


def solution(mesh):
    def local_rows(x_loc, v_loc, length_scale, out_scale):
        two_ell_sq = 2.0 * length_scale[0] * length_scale[0]
        consts = jnp.stack([(2.0 * LOG2E) / two_ell_sq, out_scale[0]])
        sx, aug, xt = pl.pallas_call(
            gather_kernel,
            out_shape=(jax.ShapeDtypeStruct((NEAR, SROWS, 128), BF), jax.ShapeDtypeStruct((NEAR, ROWS, 128), BF),
                       jax.ShapeDtypeStruct((NTGT, GROUPS, 256, 128), BF)),
            in_specs=[VM, VM],
            out_specs=(VM, VM, VM),
            scratch_shapes=[pltpu.SemaphoreType.DMA((8,)), pltpu.SemaphoreType.DMA((NEAR,)),
                            pltpu.SemaphoreType.DMA((8,)), pltpu.SemaphoreType.DMA((NTGT,))],
            compiler_params=pltpu.CompilerParams(collective_id=0, has_side_effects=True, vmem_limit_bytes=16 * 2**20),
            name="gather",
        )(x_loc, v_loc.T)
        line = sx[1:4]
        far = [lax.ppermute(line, ("col", "row"), cross_pairs(d)) for d in (1, 3, 2)]
        y_shape = jax.ShapeDtypeStruct((2, 5, 3, RHS, 256), F32)
        yn = pl.pallas_call(
            near_kernel,
            out_shape=y_shape,
            in_specs=[SM, VM, VM, VM],
            out_specs=VM,
            scratch_shapes=[pltpu.VMEM((2, 3, 256, 256), BF)],
            compiler_params=pltpu.CompilerParams(vmem_limit_bytes=16 * 2**20),
            cost_estimate=pl.CostEstimate(flops=2 * FLOPS * NEAR, bytes_accessed=2**20, transcendentals=0),
            name="near",
        )(consts, sx, aug, xt)
        yn, *far = lax.optimization_barrier((yn, *far))
        yp = pl.pallas_call(
            far_kernel,
            out_shape=y_shape,
            in_specs=[SM, VM, VM, VM, VM, VM],
            out_specs=VM,
            scratch_shapes=[pltpu.VMEM((2, 3, 256, 256), BF), pltpu.VMEM((9, ROWS, 128), BF)],
            compiler_params=pltpu.CompilerParams(vmem_limit_bytes=16 * 2**20),
            cost_estimate=pl.CostEstimate(flops=2 * FLOPS * 9, bytes_accessed=2**20, transcendentals=0),
            name="far",
        )(consts, *far, xt, yn)
        y_t = pl.pallas_call(
            reduce_kernel,
            out_shape=jax.ShapeDtypeStruct((RHS, ROWS), F32),
            in_specs=[VM],
            out_specs=VM,
            scratch_shapes=[pltpu.VMEM((4, 3, RHS, 256), F32), pltpu.VMEM((4, 3, RHS, 256), F32),
                            pltpu.VMEM((3, 3, RHS, 256), F32), pltpu.SemaphoreType.DMA((4,)), pltpu.SemaphoreType.DMA((4,)),
                            pltpu.SemaphoreType.DMA((3,)), pltpu.SemaphoreType.DMA((3,))],
            compiler_params=pltpu.CompilerParams(collective_id=1, has_side_effects=True, vmem_limit_bytes=8 * 2**20),
            name="reduce",
        )(yp)
        return y_t.T

    row_spec = P(("tasks", "row", "col"), None)
    rep_spec = P(None)
    return jax.shard_map(local_rows, mesh=mesh, in_specs=(row_spec, row_spec, rep_spec, rep_spec), out_specs=row_spec, check_vma=False)
```

```python
import functools

import jax
import jax.numpy as jnp
from jax import lax
from jax.experimental import pallas as pl
from jax.experimental.pallas import tpu as pltpu
from jax.sharding import PartitionSpec as P

BF = jnp.bfloat16
F32 = jnp.float32
ROWS = 768
FEAT = 128
RHS = 32
LINE = 4
NTGT = 8
GROUPS = 6
VROWS = GROUPS * RHS
NROWS = GROUPS * 16
NBASE = ROWS + VROWS
SROWS = ROWS + VROWS + NROWS
HALF = SROWS // 2
XROWS = 144
TILES = 3
PAIRS = 12
LOG2E = 1.4426950408889634
BIG = 3.0e38


def pieces(norm):
    half = jnp.maximum(norm * -0.5, -BIG)
    hi = half.astype(BF).astype(F32)
    rest = half - hi
    mid = rest.astype(BF).astype(F32)
    return hi, mid, rest - mid


def select(pos, at, vals):
    out = jnp.zeros_like(vals[0] + pos.astype(F32))
    for k, val in enumerate(vals):
        out = jnp.where(pos == at + k, val, out)
    return out


def position():
    col = lax.axis_index("col")
    row = lax.axis_index("row")
    return col, row // 16, (row // 4) % 4, row % 4


def device(col, z, y, x):
    return (0, col, (z % 4) * 16 + (y % 4) * 4 + x % 4)


def enter(peers):
    barrier = pltpu.get_barrier_semaphore()
    for peer in peers:
        pl.semaphore_signal(barrier, inc=1, device_id=peer, device_id_type=pl.DeviceIdType.MESH)
    pl.semaphore_wait(barrier, len(peers))


def gather_kernel(sc_ref, x_ref, v_ref, sx_ref, xt_ref, ssem, rsem, tsend, trecv):
    c, z, y, x = position()
    partner = device(1 - c, z, y, x)

    def along(d):
        return device(c, z + d * (1 - c), y + d * c, x)

    sx_ref[0, 0:ROWS, :] = x_ref[...]
    for g in range(GROUPS):
        sx_ref[0, ROWS + g * RHS : ROWS + (g + 1) * RHS, :] = v_ref[:, g * 128 : (g + 1) * 128]
    xt = jnp.transpose(x_ref[...].astype(F32))
    nrm = jnp.sum(xt * xt, axis=0, keepdims=True)
    hi, mid, low = pieces(nrm)
    pos = lax.broadcasted_iota(jnp.int32, (16, 128), 0)
    one = jnp.ones((1, 128), F32)
    for g in range(GROUPS):
        s = slice(g * 128, (g + 1) * 128)
        part = (hi[:, s], mid[:, s], low[:, s])
        sx_ref[0, NBASE + g * 16 : NBASE + (g + 1) * 16, :] = select(pos, 0, (one, one, one) + part).astype(BF)
        xt_ref[0, g, 0:FEAT, :] = xt[:, s].astype(BF)
        xt_ref[0, g, FEAT:XROWS, :] = select(pos, 0, part + (one, one, one)).astype(BF)

    enter([partner, along(1), along(3), device(c, z, y, x + 1), device(c, z, y, x + 3)])

    copies = []

    def src_part(slot, h):
        return sx_ref.at[slot, pl.ds(h * HALF, HALF), :]

    def send(src, dst, h, dev):
        cp = pltpu.make_async_remote_copy(src_part(src, h), src_part(dst, h), ssem.at[len(copies)], rsem.at[dst, h],
                                          device_id=dev, device_id_type=pl.DeviceIdType.MESH)
        cp.start()
        copies.append(cp)

    def got(slot, h):
        pltpu.make_async_remote_copy(src_part(slot, h), src_part(slot, h), ssem.at[0], rsem.at[slot, h],
                                     device_id=partner, device_id_type=pl.DeviceIdType.MESH).wait_recv()

    tcopies = []

    def tgt_part(slot, h):
        return xt_ref.at[slot, pl.ds(h * 3, 3), pl.ds(0, XROWS), :]

    def tsnd(src, dst, h, dev):
        cp = pltpu.make_async_remote_copy(tgt_part(src, h), tgt_part(dst, h), tsend.at[len(tcopies)], trecv.at[dst, h],
                                          device_id=dev, device_id_type=pl.DeviceIdType.MESH)
        cp.start()
        tcopies.append(cp)

    def tgot(slot, h):
        pltpu.make_async_remote_copy(tgt_part(slot, h), tgt_part(slot, h), tsend.at[0], trecv.at[slot, h],
                                     device_id=partner, device_id_type=pl.DeviceIdType.MESH).wait_recv()

    right = device(c, z, y, x + 1)
    left = device(c, z, y, x + 3)
    tsnd(0, 6, 0, right)
    tsnd(0, 2, 1, left)
    send(0, 3, 0, along(1))
    send(0, 1, 1, along(3))
    tsnd(0, 6, 1, right)
    tsnd(0, 2, 0, left)
    send(0, 3, 1, along(1))
    send(0, 1, 0, along(3))
    for h in range(2):
        tsnd(0, 1, h, partner)
    for t in range(NTGT):
        for g in range(GROUPS):
            xt_ref[t, g, XROWS:256, :] = jnp.zeros((256 - XROWS, 128), BF)
    got(3, 0)
    send(3, 2, 0, along(1))
    got(1, 1)
    send(1, 2, 1, along(3))
    tgot(6, 0)
    tsnd(6, 4, 0, right)
    tgot(2, 1)
    tsnd(2, 4, 1, left)
    tsnd(6, 7, 0, partner)
    tsnd(2, 3, 1, partner)
    tgot(6, 1)
    tsnd(6, 7, 1, partner)
    tgot(2, 0)
    tsnd(2, 3, 0, partner)
    got(3, 1)
    got(1, 0)
    got(2, 0)
    got(2, 1)
    for h in range(2):
        tgot(4, h)
        tsnd(4, 5, h, partner)
    for t in (1, 3, 7, 5):
        for h in range(2):
            tgot(t, h)
    for cp in copies:
        cp.wait_send()
    for cp in tcopies:
        cp.wait_send()


def product(alpha, scale, srcs, xt_ref, y_ref, tile_ref, aug_ref, eye_ref):
    piece = 64
    n_pc = 256 // piece
    per_pair = len(srcs) * TILES
    span = 24 // per_pair
    steps = span * per_pair

    def run(*accs):
        per = 3 * n_pc + span + 1
        gram = [[[accs[q * per + r * n_pc + p] for p in range(n_pc)] for r in range(3)] for q in range(2)]
        body_acc = [[accs[q * per + 3 * n_pc + w] for q in range(2)] for w in range(span)]
        tail_acc = [accs[q * per + 3 * n_pc + span] for q in range(2)]

        def acc_gram(q, u, t, p):
            rows = pl.ds((t % TILES) * 256 + p * piece, piece)
            lhs = jnp.concatenate([srcs[t // TILES][rows, :], aug_ref[t // TILES, rows, :]], axis=1)
            pltpu.matmul_acc_lhs(gram[q][u % 3][p], lhs, load_staged_rhs=0 if p == 0 else None)

        def push_x(q, pair):
            tgt = (pair // 3) * 2 + q
            ch = (pair % 3) * 2
            pltpu.matmul_push_rhs(jnp.concatenate([xt_ref[tgt, ch], xt_ref[tgt, ch + 1]], axis=1),
                                  staging_register=0, mxu_index=q)

        def push_tile(q, u):
            pltpu.matmul_push_rhs(tile_ref[q, (u - 1) % 3], staging_register=1, mxu_index=q)

        def values(q, u, p):
            half = pltpu.matmul_pop(gram[q][(u - 2) % 3][p])
            kern = (jnp.exp2(jnp.minimum(half * alpha, 0.0)) * scale).astype(BF)
            tile_ref[q, u % 3, p * piece : (p + 1) * piece, :] = kern

        def acc_y(q, t, acc):
            lo = ROWS + (t % TILES) * 2 * RHS
            src = srcs[t // TILES]
            vt = jnp.concatenate([src[pl.ds(lo, RHS), :], src[pl.ds(lo + RHS, RHS), :]], axis=1)
            pltpu.matmul_acc_lhs(acc[q], vt, load_staged_rhs=1)

        def add_y(acc, pair):
            for q in range(2):
                y_ref[q, pair // 3, pair % 3] += pltpu.matmul_pop(acc[q])

        def clear():
            for q in range(2):
                for r in range(3):
                    for p in range(n_pc):
                        pltpu.matmul_pop(gram[q][r][p])
                for acc in body_acc:
                    pltpu.matmul_pop(acc[q])
                pltpu.matmul_pop(tail_acc[q])

        def norm_columns():
            row = lax.broadcasted_iota(jnp.int32, (256, 256), 0)
            colm = lax.broadcasted_iota(jnp.int32, (256, 256), 1)
            eye_ref[...] = jnp.where(row == colm, 1.0, 0.0).astype(BF)

            def take(i):
                for p in range(n_pc):
                    cols = pltpu.matmul_pop(gram[i % 2][(i // 2) % 3][p])
                    aug_ref[i // TILES, pl.ds((i % TILES) * 256 + p * piece, piece), :] = cols[:, 0:128].astype(BF)

            for i in range(per_pair):
                src = srcs[i // TILES]
                lo = NBASE + (i % TILES) * 32
                nrm = jnp.concatenate([src[pl.ds(lo, 16), :], src[pl.ds(lo + 16, 16), :]], axis=1)
                pltpu.matmul_push_rhs(jnp.concatenate([nrm, jnp.zeros((240, 256), BF)], axis=0),
                                      staging_register=0, mxu_index=i % 2, transpose=True)
                for p in range(n_pc):
                    pltpu.matmul_acc_lhs(gram[i % 2][(i // 2) % 3][p], eye_ref[p * piece : (p + 1) * piece, :],
                                         load_staged_rhs=0 if p == 0 else None)
                if i >= 4:
                    take(i - 4)
            for i in range(per_pair - 4, per_pair):
                take(i)

        def trip(k, carry):
            old = jnp.where(k == 0, PAIRS, k * span - 1)
            for u in range(steps):
                if u < steps - 1:
                    nxt = k * span + (u + 1) // per_pair
                else:
                    nxt = jnp.minimum((k + 1) * span, PAIRS - 1)
                for q in range(2):
                    push_tile(q, u)
                for p in range(n_pc):
                    for q in range(2):
                        acc_gram(q, u, u % per_pair, p)
                        if p == 0:
                            push_x(q, nxt)
                    for q in range(2):
                        values(q, u, p)
                for q in range(2):
                    if u < 3:
                        acc_y(q, per_pair - 3 + u, tail_acc)
                    else:
                        acc_y(q, (u - 3) % per_pair, body_acc[(u - 3) // per_pair])
                if u == 1:
                    add_y(body_acc[span - 1], old)
                if u == 6:
                    add_y(tail_acc, old)
                for w in range(span - 1):
                    if u == (w + 1) * per_pair + 8:
                        add_y(body_acc[w], k * span + w)
            return carry

        clear()
        norm_columns()
        for q in range(2):
            push_x(q, 0)
        lax.fori_loop(0, PAIRS // span, trip, 0)
        for u in range(steps, steps + 3):
            for q in range(2):
                push_tile(q, u)
                if u < steps + 2:
                    for p in range(n_pc):
                        values(q, u, p)
                acc_y(q, (u - 3) % per_pair, tail_acc)
        add_y(body_acc[span - 1], PAIRS - 1)
        for q in range(2):
            acc_gram(q, 0, 0, 0)
            pltpu.matmul_pop(gram[q][0][0])
        add_y(tail_acc, PAIRS - 1)

    specs = []
    for q in range(2):
        specs += [pltpu.ACC(q)((piece, 256), F32)] * (3 * n_pc) + [pltpu.ACC(q)((RHS, 256), F32)] * (span + 1)
    pl.run_scoped(run, *specs)


def first_kernel(sc_ref, xt_ref, src_ref, y_ref, tile_ref, aug_ref, eye_ref):
    y_ref[...] = jnp.zeros_like(y_ref)
    srcs = [src_ref.at[b] for b in range(LINE)]
    product(sc_ref[0], sc_ref[1], srcs, xt_ref, y_ref, tile_ref, aug_ref, eye_ref)


def later_kernel(sc_ref, xt_ref, yin_ref, *refs):
    y_ref, tile_ref, aug_ref, eye_ref = refs[-4:]
    y_ref[...] = yin_ref[...]
    srcs = [ref.at[b] for ref in refs[:-4] for b in range(LINE)]
    product(sc_ref[0], sc_ref[1], srcs, xt_ref, y_ref, tile_ref, aug_ref, eye_ref)


def reduce_kernel(yp_ref, y_ref, part_ref, stage_ref, got_ref, psend, precv, ssem, rsem):
    c, z, y, x = position()
    partner = device(1 - c, z, y, x)
    enter([partner] + [device(c, z, y, x + d) for d in (1, 2, 3)])
    order = (2, 1, 3, 0)
    first = []
    for d in order:
        cp = pltpu.make_async_remote_copy(yp_ref.at[1, d], part_ref.at[d], psend.at[d], precv.at[d],
                                          device_id=partner, device_id_type=pl.DeviceIdType.MESH)
        cp.start()
        first.append(cp)
    second = []
    for cp, d in zip(first, order):
        cp.wait()
        stage_ref[d] = yp_ref[0, d] + part_ref[d]
        if d:
            cp2 = pltpu.make_async_remote_copy(stage_ref.at[d], got_ref.at[d - 1], ssem.at[d - 1], rsem.at[d - 1],
                                               device_id=device(c, z, y, x + d), device_id_type=pl.DeviceIdType.MESH)
            cp2.start()
            second.append(cp2)
    for cp in second:
        cp.wait()
    for ch in range(3):
        y_ref[:, ch * 256 : (ch + 1) * 256] = stage_ref[0, ch] + got_ref[0, ch] + got_ref[1, ch] + got_ref[2, ch]


def cross_pairs(shift):
    pairs = []
    for c in range(2):
        for z in range(4):
            for y in range(4):
                for x in range(4):
                    z2 = (z + shift * c) % 4
                    y2 = (y + shift * (1 - c)) % 4
                    pairs.append((c * 64 + z * 16 + y * 4 + x, c * 64 + z2 * 16 + y2 * 4 + x))
    return pairs


VM = pl.BlockSpec(memory_space=pltpu.VMEM)
SM = pl.BlockSpec(memory_space=pltpu.SMEM)
FLOPS = 2 * ROWS * ROWS * (2 * FEAT + RHS) * NTGT


def solution(mesh):
    y_shape = jax.ShapeDtypeStruct((2, 5, 3, RHS, 256), F32)

    def product_call(kernel, consts, xt, args, lines):
        return pl.pallas_call(
            kernel,
            out_shape=y_shape,
            in_specs=[SM] + [VM] * (1 + len(args)),
            out_specs=VM,
            scratch_shapes=[pltpu.VMEM((2, 3, 256, 256), BF), pltpu.VMEM((lines * LINE, ROWS, 128), BF),
                            pltpu.VMEM((256, 256), BF)],
            compiler_params=pltpu.CompilerParams(vmem_limit_bytes=16 * 2**20),
            cost_estimate=pl.CostEstimate(flops=2 * FLOPS * LINE * lines, bytes_accessed=2**20, transcendentals=0),
            name="product",
        )(consts, xt, *args)

    def local_rows(x_loc, v_loc, length_scale, out_scale):
        two_ell_sq = 2.0 * length_scale[0] * length_scale[0]
        consts = jnp.stack([(2.0 * LOG2E) / two_ell_sq, out_scale[0]])
        line, xt = pl.pallas_call(
            gather_kernel,
            out_shape=(jax.ShapeDtypeStruct((LINE, SROWS, 128), BF), jax.ShapeDtypeStruct((NTGT, GROUPS, 256, 128), BF)),
            in_specs=[SM, VM, VM],
            out_specs=(VM, VM),
            scratch_shapes=[pltpu.SemaphoreType.DMA((6,)), pltpu.SemaphoreType.DMA((LINE, 2)),
                            pltpu.SemaphoreType.DMA((14,)), pltpu.SemaphoreType.DMA((NTGT, 2))],
            compiler_params=pltpu.CompilerParams(collective_id=0, has_side_effects=True, vmem_limit_bytes=16 * 2**20),
            name="gather",
        )(consts, x_loc, v_loc.T)
        up, down = [lax.ppermute(line, ("col", "row"), cross_pairs(d)) for d in (1, 3)]
        y1 = product_call(first_kernel, consts, xt, (line,), 1)
        y1, up, down, line = lax.optimization_barrier((y1, up, down, line))
        across = lax.ppermute(line, ("col", "row"), cross_pairs(2))
        y2 = product_call(later_kernel, consts, xt, (y1, up, down), 2)
        y2, across = lax.optimization_barrier((y2, across))
        yp = product_call(later_kernel, consts, xt, (y2, across), 1)
        y_t = pl.pallas_call(
            reduce_kernel,
            out_shape=jax.ShapeDtypeStruct((RHS, ROWS), F32),
            in_specs=[VM],
            out_specs=VM,
            scratch_shapes=[pltpu.VMEM((4, 3, RHS, 256), F32), pltpu.VMEM((4, 3, RHS, 256), F32),
                            pltpu.VMEM((3, 3, RHS, 256), F32), pltpu.SemaphoreType.DMA((4,)), pltpu.SemaphoreType.DMA((4,)),
                            pltpu.SemaphoreType.DMA((3,)), pltpu.SemaphoreType.DMA((3,))],
            compiler_params=pltpu.CompilerParams(collective_id=1, has_side_effects=True, vmem_limit_bytes=8 * 2**20),
            name="reduce",
        )(yp)
        return y_t.T

    row_spec = P(("tasks", "row", "col"), None)
    rep_spec = P(None)
    return jax.shard_map(local_rows, mesh=mesh, in_specs=(row_spec, row_spec, rep_spec, rep_spec), out_specs=row_spec, check_vma=False)
```

```python
import functools

import jax
import jax.numpy as jnp
from jax import lax
from jax.experimental import pallas as pl
from jax.experimental.pallas import tpu as pltpu
from jax.sharding import PartitionSpec as P

BF = jnp.bfloat16
F32 = jnp.float32
ROWS = 768
FEAT = 128
RHS = 32
LINE = 4
NTGT = 8
GROUPS = 6
VROWS = GROUPS * RHS
NROWS = GROUPS * 16
NBASE = ROWS + VROWS
SROWS = ROWS + VROWS + NROWS
HALF = SROWS // 2
XROWS = 144
TILES = 3
PAIRS = 12
LOG2E = 1.4426950408889634
BIG = 3.0e38


def pieces(norm):
    half = jnp.maximum(norm * -0.5, -BIG)
    hi = half.astype(BF).astype(F32)
    rest = half - hi
    mid = rest.astype(BF).astype(F32)
    return hi, mid, rest - mid


def select(pos, at, vals):
    out = jnp.zeros_like(vals[0] + pos.astype(F32))
    for k, val in enumerate(vals):
        out = jnp.where(pos == at + k, val, out)
    return out


def position():
    col = lax.axis_index("col")
    row = lax.axis_index("row")
    return col, row // 16, (row // 4) % 4, row % 4


def device(col, z, y, x):
    return (0, col, (z % 4) * 16 + (y % 4) * 4 + x % 4)


def greet(peers):
    barrier = pltpu.get_barrier_semaphore()
    for peer in peers:
        pl.semaphore_signal(barrier, inc=1, device_id=peer, device_id_type=pl.DeviceIdType.MESH)


def enter(peers):
    pl.semaphore_wait(pltpu.get_barrier_semaphore(), len(peers))


def gather_kernel(sc_ref, x_ref, v_ref, sx_ref, xt_ref, ssem, rsem, tsend, trecv):
    c, z, y, x = position()
    partner = device(1 - c, z, y, x)

    def along(d):
        return device(c, z + d * (1 - c), y + d * c, x)

    peers = [partner, along(1), along(3), device(c, z, y, x + 1), device(c, z, y, x + 3)]
    greet(peers)
    sx_ref[0, 0:ROWS, :] = x_ref[...]
    for g in range(GROUPS):
        sx_ref[0, ROWS + g * RHS : ROWS + (g + 1) * RHS, :] = v_ref[:, g * 128 : (g + 1) * 128]
    for t in range(NTGT):
        for g in range(GROUPS):
            xt_ref[t, g, XROWS:256, :] = jnp.zeros((256 - XROWS, 128), BF)
    xt = jnp.transpose(x_ref[...].astype(F32))
    nrm = jnp.sum(xt * xt, axis=0, keepdims=True)
    hi, mid, low = pieces(nrm)
    pos = lax.broadcasted_iota(jnp.int32, (16, 128), 0)
    one = jnp.ones((1, 128), F32)
    for g in range(GROUPS):
        s = slice(g * 128, (g + 1) * 128)
        part = (hi[:, s], mid[:, s], low[:, s])
        sx_ref[0, NBASE + g * 16 : NBASE + (g + 1) * 16, :] = select(pos, 0, (one, one, one) + part).astype(BF)
        xt_ref[0, g, 0:FEAT, :] = xt[:, s].astype(BF)
        xt_ref[0, g, FEAT:XROWS, :] = select(pos, 0, part + (one, one, one)).astype(BF)

    enter(peers)

    copies = []

    def src_part(slot, h):
        return sx_ref.at[slot, pl.ds(h * HALF, HALF), :]

    def send(src, dst, h, dev):
        cp = pltpu.make_async_remote_copy(src_part(src, h), src_part(dst, h), ssem.at[len(copies)], rsem.at[dst, h],
                                          device_id=dev, device_id_type=pl.DeviceIdType.MESH)
        cp.start()
        copies.append(cp)

    def got(slot, h):
        pltpu.make_async_remote_copy(src_part(slot, h), src_part(slot, h), ssem.at[0], rsem.at[slot, h],
                                     device_id=partner, device_id_type=pl.DeviceIdType.MESH).wait_recv()

    tcopies = []

    def tgt_part(slot, h):
        return xt_ref.at[slot, pl.ds(h * 3, 3), pl.ds(0, XROWS), :]

    def tsnd(src, dst, h, dev):
        cp = pltpu.make_async_remote_copy(tgt_part(src, h), tgt_part(dst, h), tsend.at[len(tcopies)], trecv.at[dst, h],
                                          device_id=dev, device_id_type=pl.DeviceIdType.MESH)
        cp.start()
        tcopies.append(cp)

    def tgot(slot, h):
        pltpu.make_async_remote_copy(tgt_part(slot, h), tgt_part(slot, h), tsend.at[0], trecv.at[slot, h],
                                     device_id=partner, device_id_type=pl.DeviceIdType.MESH).wait_recv()

    right = device(c, z, y, x + 1)
    left = device(c, z, y, x + 3)
    tsnd(0, 6, 0, right)
    tsnd(0, 2, 1, left)
    send(0, 3, 0, along(1))
    send(0, 1, 1, along(3))
    tsnd(0, 6, 1, right)
    tsnd(0, 2, 0, left)
    send(0, 3, 1, along(1))
    send(0, 1, 0, along(3))
    for h in range(2):
        tsnd(0, 1, h, partner)
    got(3, 0)
    send(3, 2, 0, along(1))
    got(1, 1)
    send(1, 2, 1, along(3))
    tgot(6, 0)
    tsnd(6, 4, 0, right)
    tgot(2, 1)
    tsnd(2, 4, 1, left)
    tsnd(6, 7, 0, partner)
    tsnd(2, 3, 1, partner)
    tgot(6, 1)
    tsnd(6, 7, 1, partner)
    tgot(2, 0)
    tsnd(2, 3, 0, partner)
    got(3, 1)
    got(1, 0)
    got(2, 0)
    got(2, 1)
    for h in range(2):
        tgot(4, h)
        tsnd(4, 5, h, partner)
    for t in (1, 3, 7, 5):
        for h in range(2):
            tgot(t, h)
    for cp in copies:
        cp.wait_send()
    for cp in tcopies:
        cp.wait_send()


def product(alpha, scale, srcs, xt_ref, y_ref, tile_ref, aug_ref, eye_ref):
    piece = 64
    n_pc = 256 // piece
    per_pair = len(srcs) * TILES
    span = 48 // per_pair
    steps = span * per_pair

    def run(*accs):
        per = 3 * n_pc + span + 1
        gram = [[[accs[q * per + r * n_pc + p] for p in range(n_pc)] for r in range(3)] for q in range(2)]
        body_acc = [[accs[q * per + 3 * n_pc + w] for q in range(2)] for w in range(span)]
        tail_acc = [accs[q * per + 3 * n_pc + span] for q in range(2)]

        def acc_gram(q, u, t, p):
            rows = pl.ds((t % TILES) * 256 + p * piece, piece)
            lhs = jnp.concatenate([srcs[t // TILES][rows, :], aug_ref[t // TILES, rows, :]], axis=1)
            pltpu.matmul_acc_lhs(gram[q][u % 3][p], lhs, load_staged_rhs=0 if p == 0 else None)

        def push_x(q, pair):
            tgt = (pair // 3) * 2 + q
            ch = (pair % 3) * 2
            pltpu.matmul_push_rhs(jnp.concatenate([xt_ref[tgt, ch], xt_ref[tgt, ch + 1]], axis=1),
                                  staging_register=0, mxu_index=q)

        def push_tile(q, u):
            pltpu.matmul_push_rhs(tile_ref[q, (u - 1) % 3], staging_register=1, mxu_index=q)

        def values(q, u, p):
            half = pltpu.matmul_pop(gram[q][(u - 2) % 3][p])
            kern = (jnp.exp2(jnp.minimum(half * alpha, 0.0)) * scale).astype(BF)
            tile_ref[q, u % 3, p * piece : (p + 1) * piece, :] = kern

        def acc_y(q, t, acc):
            lo = ROWS + (t % TILES) * 2 * RHS
            src = srcs[t // TILES]
            vt = jnp.concatenate([src[pl.ds(lo, RHS), :], src[pl.ds(lo + RHS, RHS), :]], axis=1)
            pltpu.matmul_acc_lhs(acc[q], vt, load_staged_rhs=1)

        def add_y(acc, pair):
            for q in range(2):
                y_ref[q, pair // 3, pair % 3] += pltpu.matmul_pop(acc[q])

        def clear():
            for q in range(2):
                for r in range(3):
                    for p in range(n_pc):
                        pltpu.matmul_pop(gram[q][r][p])
                for acc in body_acc:
                    pltpu.matmul_pop(acc[q])
                pltpu.matmul_pop(tail_acc[q])

        def norm_columns():
            row = lax.broadcasted_iota(jnp.int32, (256, 256), 0)
            colm = lax.broadcasted_iota(jnp.int32, (256, 256), 1)
            eye_ref[...] = jnp.where(row == colm, 1.0, 0.0).astype(BF)

            def take(i):
                for p in range(n_pc):
                    cols = pltpu.matmul_pop(gram[i % 2][(i // 2) % 3][p])
                    aug_ref[i // TILES, pl.ds((i % TILES) * 256 + p * piece, piece), :] = cols[:, 0:128].astype(BF)

            for i in range(per_pair):
                src = srcs[i // TILES]
                lo = NBASE + (i % TILES) * 32
                nrm = jnp.concatenate([src[pl.ds(lo, 16), :], src[pl.ds(lo + 16, 16), :]], axis=1)
                pltpu.matmul_push_rhs(jnp.concatenate([nrm, jnp.zeros((240, 256), BF)], axis=0),
                                      staging_register=0, mxu_index=i % 2, transpose=True)
                for p in range(n_pc):
                    pltpu.matmul_acc_lhs(gram[i % 2][(i // 2) % 3][p], eye_ref[p * piece : (p + 1) * piece, :],
                                         load_staged_rhs=0 if p == 0 else None)
                if i >= 4:
                    take(i - 4)
            for i in range(per_pair - 4, per_pair):
                take(i)

        def trip(k, carry):
            old = jnp.where(k == 0, PAIRS, k * span - 1)
            for u in range(steps):
                if u < steps - 1:
                    nxt = k * span + (u + 1) // per_pair
                else:
                    nxt = jnp.minimum((k + 1) * span, PAIRS - 1)
                for q in range(2):
                    push_tile(q, u)
                for p in range(n_pc):
                    for q in range(2):
                        acc_gram(q, u, u % per_pair, p)
                        if p == 0:
                            push_x(q, nxt)
                    for q in range(2):
                        values(q, u, p)
                for q in range(2):
                    if u < 3:
                        acc_y(q, per_pair - 3 + u, tail_acc)
                    else:
                        acc_y(q, (u - 3) % per_pair, body_acc[(u - 3) // per_pair])
                if u == 1:
                    add_y(body_acc[span - 1], old)
                if u == 6:
                    add_y(tail_acc, old)
                for w in range(span - 1):
                    if u == (w + 1) * per_pair + 8:
                        add_y(body_acc[w], k * span + w)
            return carry

        clear()
        norm_columns()
        for q in range(2):
            push_x(q, 0)
        lax.fori_loop(0, PAIRS // span, trip, 0)
        for u in range(steps, steps + 3):
            for q in range(2):
                push_tile(q, u)
                if u < steps + 2:
                    for p in range(n_pc):
                        values(q, u, p)
                acc_y(q, (u - 3) % per_pair, tail_acc)
        add_y(body_acc[span - 1], PAIRS - 1)
        for q in range(2):
            acc_gram(q, 0, 0, 0)
            pltpu.matmul_pop(gram[q][0][0])
        add_y(tail_acc, PAIRS - 1)

    specs = []
    for q in range(2):
        specs += [pltpu.ACC(q)((piece, 256), F32)] * (3 * n_pc) + [pltpu.ACC(q)((RHS, 256), F32)] * (span + 1)
    pl.run_scoped(run, *specs)


def first_kernel(sc_ref, xt_ref, src_ref, y_ref, tile_ref, aug_ref, eye_ref):
    y_ref[...] = jnp.zeros_like(y_ref)
    srcs = [src_ref.at[b] for b in range(LINE)]
    product(sc_ref[0], sc_ref[1], srcs, xt_ref, y_ref, tile_ref, aug_ref, eye_ref)


def later_kernel(sc_ref, xt_ref, yin_ref, *refs):
    y_ref, tile_ref, aug_ref, eye_ref = refs[-4:]
    y_ref[...] = yin_ref[...]
    srcs = [ref.at[b] for ref in refs[:-4] for b in range(LINE)]
    product(sc_ref[0], sc_ref[1], srcs, xt_ref, y_ref, tile_ref, aug_ref, eye_ref)


def reduce_kernel(yp_ref, y_ref, part_ref, tot_ref, hop_ref, sum_ref, got_ref, psend, precv, ssem, rsem):
    c, z, y, x = position()
    partner = device(1 - c, z, y, x)
    right = device(c, z, y, x + 1)
    left = device(c, z, y, x + 3)
    peers = [partner, right, left]
    greet(peers)
    enter(peers)
    up = pl.ds(0, RHS // 2)
    down = pl.ds(RHS // 2, RHS // 2)
    copies = []

    def send(src, dst, k, dev):
        cp = pltpu.make_async_remote_copy(src, dst, ssem.at[k], rsem.at[k], device_id=dev,
                                          device_id_type=pl.DeviceIdType.MESH)
        cp.start()
        copies.append(cp)

    first = {}
    for d in (2, 1, 3, 0):
        first[d] = pltpu.make_async_remote_copy(yp_ref.at[1, d], part_ref.at[d], psend.at[d], precv.at[d],
                                                device_id=partner, device_id_type=pl.DeviceIdType.MESH)
        first[d].start()

    def total(d):
        first[d].wait()
        tot_ref[d] = yp_ref[0, d] + part_ref[d]

    total(2)
    send(tot_ref.at[2, :, up, :], hop_ref.at[0], 0, right)
    send(tot_ref.at[2, :, down, :], hop_ref.at[1], 1, left)
    total(1)
    send(tot_ref.at[1, :, down, :], got_ref.at[0], 2, right)
    total(3)
    send(tot_ref.at[3, :, up, :], got_ref.at[1], 3, left)
    total(0)
    copies[0].wait_recv()
    sum_ref[0] = hop_ref[0] + tot_ref[1, :, 0 : RHS // 2, :]
    send(sum_ref.at[0], got_ref.at[2], 4, right)
    copies[1].wait_recv()
    sum_ref[1] = hop_ref[1] + tot_ref[3, :, RHS // 2 : RHS, :]
    send(sum_ref.at[1], got_ref.at[3], 5, left)
    for k in (2, 3, 4, 5):
        copies[k].wait_recv()
    for ch in range(3):
        cols = slice(ch * 256, (ch + 1) * 256)
        y_ref[0 : RHS // 2, cols] = tot_ref[0, ch, 0 : RHS // 2, :] + got_ref[1, ch] + got_ref[2, ch]
        y_ref[RHS // 2 : RHS, cols] = tot_ref[0, ch, RHS // 2 : RHS, :] + got_ref[0, ch] + got_ref[3, ch]
    for cp in copies:
        cp.wait_send()


def cross_pairs(shift):
    pairs = []
    for c in range(2):
        for z in range(4):
            for y in range(4):
                for x in range(4):
                    z2 = (z + shift * c) % 4
                    y2 = (y + shift * (1 - c)) % 4
                    pairs.append((c * 64 + z * 16 + y * 4 + x, c * 64 + z2 * 16 + y2 * 4 + x))
    return pairs


VM = pl.BlockSpec(memory_space=pltpu.VMEM)
SM = pl.BlockSpec(memory_space=pltpu.SMEM)
FLOPS = 2 * ROWS * ROWS * (2 * FEAT + RHS) * NTGT


def solution(mesh):
    y_shape = jax.ShapeDtypeStruct((2, 5, 3, RHS, 256), F32)

    def product_call(kernel, consts, xt, args, lines):
        return pl.pallas_call(
            kernel,
            out_shape=y_shape,
            in_specs=[SM] + [VM] * (1 + len(args)),
            out_specs=VM,
            scratch_shapes=[pltpu.VMEM((2, 3, 256, 256), BF), pltpu.VMEM((lines * LINE, ROWS, 128), BF),
                            pltpu.VMEM((256, 256), BF)],
            compiler_params=pltpu.CompilerParams(vmem_limit_bytes=16 * 2**20),
            cost_estimate=pl.CostEstimate(flops=2 * FLOPS * LINE * lines, bytes_accessed=2**20, transcendentals=0),
            name="product",
        )(consts, xt, *args)

    def local_rows(x_loc, v_loc, length_scale, out_scale):
        two_ell_sq = 2.0 * length_scale[0] * length_scale[0]
        consts = jnp.stack([(2.0 * LOG2E) / two_ell_sq, out_scale[0]])
        line, xt = pl.pallas_call(
            gather_kernel,
            out_shape=(jax.ShapeDtypeStruct((LINE, SROWS, 128), BF), jax.ShapeDtypeStruct((NTGT, GROUPS, 256, 128), BF)),
            in_specs=[SM, VM, VM],
            out_specs=(VM, VM),
            scratch_shapes=[pltpu.SemaphoreType.DMA((6,)), pltpu.SemaphoreType.DMA((LINE, 2)),
                            pltpu.SemaphoreType.DMA((14,)), pltpu.SemaphoreType.DMA((NTGT, 2))],
            compiler_params=pltpu.CompilerParams(collective_id=0, has_side_effects=True, vmem_limit_bytes=16 * 2**20),
            name="gather",
        )(consts, x_loc, v_loc.T)
        up, down = [lax.ppermute(line, ("col", "row"), cross_pairs(d)) for d in (1, 3)]
        y1 = product_call(first_kernel, consts, xt, (line,), 1)
        y1, up, down, line = lax.optimization_barrier((y1, up, down, line))
        across = lax.ppermute(line, ("col", "row"), cross_pairs(2))
        y2 = product_call(later_kernel, consts, xt, (y1, up, down), 2)
        y2, across = lax.optimization_barrier((y2, across))
        yp = product_call(later_kernel, consts, xt, (y2, across), 1)
        y_t = pl.pallas_call(
            reduce_kernel,
            out_shape=jax.ShapeDtypeStruct((RHS, ROWS), F32),
            in_specs=[VM],
            out_specs=VM,
            scratch_shapes=[pltpu.VMEM((4, 3, RHS, 256), F32), pltpu.VMEM((4, 3, RHS, 256), F32),
                            pltpu.VMEM((2, 3, RHS // 2, 256), F32), pltpu.VMEM((2, 3, RHS // 2, 256), F32),
                            pltpu.VMEM((4, 3, RHS // 2, 256), F32), pltpu.SemaphoreType.DMA((4,)),
                            pltpu.SemaphoreType.DMA((4,)), pltpu.SemaphoreType.DMA((6,)), pltpu.SemaphoreType.DMA((6,))],
            compiler_params=pltpu.CompilerParams(collective_id=1, has_side_effects=True, vmem_limit_bytes=8 * 2**20),
            name="reduce",
        )(yp)
        return y_t.T

    row_spec = P(("tasks", "row", "col"), None)
    rep_spec = P(None)
    return jax.shard_map(local_rows, mesh=mesh, in_specs=(row_spec, row_spec, rep_spec, rep_spec), out_specs=row_spec, check_vma=False)
```

```python
import functools

import jax
import jax.numpy as jnp
from jax import lax
from jax.experimental import pallas as pl
from jax.experimental.pallas import tpu as pltpu
from jax.sharding import PartitionSpec as P

BF = jnp.bfloat16
F32 = jnp.float32
ROWS = 768
FEAT = 128
RHS = 32
LINE = 3
NTGT = 8
GROUPS = 6
VROWS = GROUPS * RHS
NROWS = GROUPS * 16
NBASE = ROWS + VROWS
SROWS = ROWS + VROWS + NROWS
HALF = SROWS // 2
XROWS = 144
TILES = 3
PAIRS = 12
LOG2E = 1.4426950408889634
BIG = 3.0e38


def pieces(norm):
    half = jnp.maximum(norm * -0.5, -BIG)
    hi = half.astype(BF).astype(F32)
    rest = half - hi
    mid = rest.astype(BF).astype(F32)
    return hi, mid, rest - mid


def select(pos, at, vals):
    out = jnp.zeros_like(vals[0] + pos.astype(F32))
    for k, val in enumerate(vals):
        out = jnp.where(pos == at + k, val, out)
    return out


def position():
    col = lax.axis_index("col")
    row = lax.axis_index("row")
    return col, row // 16, (row // 4) % 4, row % 4


def device(col, z, y, x):
    return (0, col, (z % 4) * 16 + (y % 4) * 4 + x % 4)


def greet(peers):
    barrier = pltpu.get_barrier_semaphore()
    for peer in peers:
        pl.semaphore_signal(barrier, inc=1, device_id=peer, device_id_type=pl.DeviceIdType.MESH)


def enter(peers):
    pl.semaphore_wait(pltpu.get_barrier_semaphore(), len(peers))


def gather_kernel(sc_ref, x_ref, v_ref, own_ref, cross_ref, line_ref, xt_ref, ssem, rsem, csend, crecv, tsend, trecv):
    c, z, y, x = position()
    partner = device(1 - c, z, y, x)

    def along(d):
        return device(c, z + d * (1 - c), y + d * c, x)

    def across(d):
        return device(c, z + d * c, y + d * (1 - c), x)

    peers = [partner, along(1), along(3), across(1), across(3), device(c, z, y, x + 1), device(c, z, y, x + 3)]
    greet(peers)
    own_ref[0, 0:ROWS, :] = x_ref[...]
    for g in range(GROUPS):
        own_ref[0, ROWS + g * RHS : ROWS + (g + 1) * RHS, :] = v_ref[:, g * 128 : (g + 1) * 128]
    for t in range(NTGT):
        for g in range(GROUPS):
            xt_ref[t, g, XROWS:256, :] = jnp.zeros((256 - XROWS, 128), BF)
    xt = jnp.transpose(x_ref[...].astype(F32))
    nrm = jnp.sum(xt * xt, axis=0, keepdims=True)
    hi, mid, low = pieces(nrm)
    pos = lax.broadcasted_iota(jnp.int32, (16, 128), 0)
    one = jnp.ones((1, 128), F32)
    for g in range(GROUPS):
        s = slice(g * 128, (g + 1) * 128)
        part = (hi[:, s], mid[:, s], low[:, s])
        own_ref[0, NBASE + g * 16 : NBASE + (g + 1) * 16, :] = select(pos, 0, (one, one, one) + part).astype(BF)
        xt_ref[0, g, 0:FEAT, :] = xt[:, s].astype(BF)
        xt_ref[0, g, FEAT:XROWS, :] = select(pos, 0, part + (one, one, one)).astype(BF)

    enter(peers)

    copies = []

    def src_part(slot, h):
        ref = own_ref.at[0] if slot == 0 else line_ref.at[slot - 1]
        return ref.at[pl.ds(h * HALF, HALF), :]

    def send(src, dst, h, dev):
        cp = pltpu.make_async_remote_copy(src_part(src, h), src_part(dst, h), ssem.at[len(copies)], rsem.at[dst - 1, h],
                                          device_id=dev, device_id_type=pl.DeviceIdType.MESH)
        cp.start()
        copies.append(cp)

    def got(slot, h):
        pltpu.make_async_remote_copy(src_part(slot, h), src_part(slot, h), ssem.at[0], rsem.at[slot - 1, h],
                                     device_id=partner, device_id_type=pl.DeviceIdType.MESH).wait_recv()

    crosses = []

    def side(k, dev):
        cp = pltpu.make_async_remote_copy(own_ref.at[0], cross_ref.at[k], csend.at[k], crecv.at[k],
                                          device_id=dev, device_id_type=pl.DeviceIdType.MESH)
        cp.start()
        crosses.append(cp)

    tcopies = []

    def tgt_part(slot, h):
        return xt_ref.at[slot, pl.ds(h * 3, 3), pl.ds(0, XROWS), :]

    def tsnd(src, dst, h, dev):
        cp = pltpu.make_async_remote_copy(tgt_part(src, h), tgt_part(dst, h), tsend.at[len(tcopies)], trecv.at[dst, h],
                                          device_id=dev, device_id_type=pl.DeviceIdType.MESH)
        cp.start()
        tcopies.append(cp)

    def tgot(slot, h):
        pltpu.make_async_remote_copy(tgt_part(slot, h), tgt_part(slot, h), tsend.at[0], trecv.at[slot, h],
                                     device_id=partner, device_id_type=pl.DeviceIdType.MESH).wait_recv()

    right = device(c, z, y, x + 1)
    left = device(c, z, y, x + 3)
    tsnd(0, 6, 0, right)
    tsnd(0, 2, 1, left)
    send(0, 3, 0, along(1))
    send(0, 1, 1, along(3))
    tsnd(0, 6, 1, right)
    tsnd(0, 2, 0, left)
    send(0, 3, 1, along(1))
    send(0, 1, 0, along(3))
    for h in range(2):
        tsnd(0, 1, h, partner)
    side(1, across(1))
    side(0, across(3))
    got(3, 0)
    send(3, 2, 0, along(1))
    got(1, 1)
    send(1, 2, 1, along(3))
    tgot(6, 0)
    tsnd(6, 4, 0, right)
    tgot(2, 1)
    tsnd(2, 4, 1, left)
    tsnd(6, 7, 0, partner)
    tsnd(2, 3, 1, partner)
    tgot(6, 1)
    tsnd(6, 7, 1, partner)
    tgot(2, 0)
    tsnd(2, 3, 0, partner)
    got(3, 1)
    got(1, 0)
    got(2, 0)
    got(2, 1)
    for h in range(2):
        tgot(4, h)
        tsnd(4, 5, h, partner)
    for t in (1, 3, 7, 5):
        for h in range(2):
            tgot(t, h)
    for cp in crosses:
        cp.wait()
    for cp in copies:
        cp.wait_send()
    for cp in tcopies:
        cp.wait_send()


def product(alpha, scale, srcs, xt_ref, y_ref, tile_ref, aug_ref, eye_ref):
    piece = 64
    n_pc = 256 // piece
    per_pair = len(srcs) * TILES
    span = 48 // per_pair
    steps = span * per_pair

    def run(*accs):
        per = 3 * n_pc + span + 1
        gram = [[[accs[q * per + r * n_pc + p] for p in range(n_pc)] for r in range(3)] for q in range(2)]
        body_acc = [[accs[q * per + 3 * n_pc + w] for q in range(2)] for w in range(span)]
        tail_acc = [accs[q * per + 3 * n_pc + span] for q in range(2)]

        def acc_gram(q, u, t, p):
            rows = pl.ds((t % TILES) * 256 + p * piece, piece)
            lhs = jnp.concatenate([srcs[t // TILES][rows, :], aug_ref[t // TILES, rows, :]], axis=1)
            pltpu.matmul_acc_lhs(gram[q][u % 3][p], lhs, load_staged_rhs=0 if p == 0 else None)

        def push_x(q, pair):
            tgt = (pair // 3) * 2 + q
            ch = (pair % 3) * 2
            pltpu.matmul_push_rhs(jnp.concatenate([xt_ref[tgt, ch], xt_ref[tgt, ch + 1]], axis=1),
                                  staging_register=0, mxu_index=q)

        def push_tile(q, u):
            pltpu.matmul_push_rhs(tile_ref[q, (u - 1) % 3], staging_register=1, mxu_index=q)

        def values(q, u, p):
            half = pltpu.matmul_pop(gram[q][(u - 2) % 3][p])
            kern = (jnp.exp2(jnp.minimum(half * alpha, 0.0)) * scale).astype(BF)
            tile_ref[q, u % 3, p * piece : (p + 1) * piece, :] = kern

        def acc_y(q, t, acc):
            lo = ROWS + (t % TILES) * 2 * RHS
            src = srcs[t // TILES]
            vt = jnp.concatenate([src[pl.ds(lo, RHS), :], src[pl.ds(lo + RHS, RHS), :]], axis=1)
            pltpu.matmul_acc_lhs(acc[q], vt, load_staged_rhs=1)

        def add_y(acc, pair):
            for q in range(2):
                y_ref[q, pair // 3, pair % 3] += pltpu.matmul_pop(acc[q])

        def clear():
            for q in range(2):
                for r in range(3):
                    for p in range(n_pc):
                        pltpu.matmul_pop(gram[q][r][p])
                for acc in body_acc:
                    pltpu.matmul_pop(acc[q])
                pltpu.matmul_pop(tail_acc[q])

        def norm_columns():
            row = lax.broadcasted_iota(jnp.int32, (256, 256), 0)
            colm = lax.broadcasted_iota(jnp.int32, (256, 256), 1)
            eye_ref[...] = jnp.where(row == colm, 1.0, 0.0).astype(BF)

            def take(n):
                for p in range(n_pc):
                    cols = pltpu.matmul_pop(gram[n % 2][(n // 2) % 3][p])
                    for h in range(2):
                        i = 2 * n + h
                        rows = pl.ds((i % TILES) * 256 + p * piece, piece)
                        aug_ref[i // TILES, rows, :] = cols[:, h * 128 : (h + 1) * 128].astype(BF)

            blank = jnp.zeros((112, 256), BF)
            count = per_pair // 2
            for n in range(count):
                rows = []
                for i in (2 * n, 2 * n + 1):
                    src = srcs[i // TILES]
                    lo = NBASE + (i % TILES) * 32
                    rows += [jnp.concatenate([src[pl.ds(lo, 16), :], src[pl.ds(lo + 16, 16), :]], axis=1), blank]
                pltpu.matmul_push_rhs(jnp.concatenate(rows, axis=0), staging_register=0, mxu_index=n % 2, transpose=True)
                for p in range(n_pc):
                    pltpu.matmul_acc_lhs(gram[n % 2][(n // 2) % 3][p], eye_ref[p * piece : (p + 1) * piece, :],
                                         load_staged_rhs=0 if p == 0 else None)
                if n >= 4:
                    take(n - 4)
            for n in range(count - 4, count):
                take(n)

        def trip(k, carry):
            old = jnp.where(k == 0, PAIRS, k * span - 1)
            for u in range(steps):
                if u < steps - 1:
                    nxt = k * span + (u + 1) // per_pair
                else:
                    nxt = jnp.minimum((k + 1) * span, PAIRS - 1)
                for q in range(2):
                    push_tile(q, u)
                for p in range(n_pc):
                    for q in range(2):
                        acc_gram(q, u, u % per_pair, p)
                        if p == 0:
                            push_x(q, nxt)
                    for q in range(2):
                        values(q, u, p)
                for q in range(2):
                    if u < 3:
                        acc_y(q, per_pair - 3 + u, tail_acc)
                    else:
                        acc_y(q, (u - 3) % per_pair, body_acc[(u - 3) // per_pair])
                if u == 1:
                    add_y(body_acc[span - 1], old)
                if u == 6:
                    add_y(tail_acc, old)
                for w in range(span - 1):
                    if u == (w + 1) * per_pair + 8:
                        add_y(body_acc[w], k * span + w)
            return carry

        clear()
        norm_columns()
        for q in range(2):
            push_x(q, 0)
        lax.fori_loop(0, PAIRS // span, trip, 0)
        for u in range(steps, steps + 3):
            for q in range(2):
                push_tile(q, u)
                if u < steps + 2:
                    for p in range(n_pc):
                        values(q, u, p)
                acc_y(q, (u - 3) % per_pair, tail_acc)
        add_y(body_acc[span - 1], PAIRS - 1)
        for q in range(2):
            acc_gram(q, 0, 0, 0)
            pltpu.matmul_pop(gram[q][0][0])
        add_y(tail_acc, PAIRS - 1)

    specs = []
    for q in range(2):
        specs += [pltpu.ACC(q)((piece, 256), F32)] * (3 * n_pc) + [pltpu.ACC(q)((RHS, 256), F32)] * (span + 1)
    pl.run_scoped(run, *specs)


def first_kernel(sc_ref, xt_ref, *refs):
    y_ref, tile_ref, aug_ref, eye_ref = refs[-4:]
    y_ref[...] = jnp.zeros_like(y_ref)
    srcs = [ref.at[b] for ref in refs[:-4] for b in range(ref.shape[0])]
    product(sc_ref[0], sc_ref[1], srcs, xt_ref, y_ref, tile_ref, aug_ref, eye_ref)


def later_kernel(sc_ref, xt_ref, yin_ref, *refs):
    y_ref, tile_ref, aug_ref, eye_ref = refs[-4:]
    y_ref[...] = yin_ref[...]
    srcs = [ref.at[b] for ref in refs[:-4] for b in range(ref.shape[0])]
    product(sc_ref[0], sc_ref[1], srcs, xt_ref, y_ref, tile_ref, aug_ref, eye_ref)


def reduce_kernel(yp_ref, y_ref, part_ref, tot_ref, hop_ref, sum_ref, got_ref, psend, precv, ssem, rsem):
    c, z, y, x = position()
    partner = device(1 - c, z, y, x)
    right = device(c, z, y, x + 1)
    left = device(c, z, y, x + 3)
    peers = [partner, right, left]
    greet(peers)
    enter(peers)
    up = pl.ds(0, RHS // 2)
    down = pl.ds(RHS // 2, RHS // 2)
    copies = []

    def send(src, dst, k, dev):
        cp = pltpu.make_async_remote_copy(src, dst, ssem.at[k], rsem.at[k], device_id=dev,
                                          device_id_type=pl.DeviceIdType.MESH)
        cp.start()
        copies.append(cp)

    first = {}
    for d in (2, 1, 3, 0):
        first[d] = pltpu.make_async_remote_copy(yp_ref.at[1, d], part_ref.at[d], psend.at[d], precv.at[d],
                                                device_id=partner, device_id_type=pl.DeviceIdType.MESH)
        first[d].start()

    def total(d):
        first[d].wait()
        tot_ref[d] = yp_ref[0, d] + part_ref[d]

    total(2)
    send(tot_ref.at[2, :, up, :], hop_ref.at[0], 0, right)
    send(tot_ref.at[2, :, down, :], hop_ref.at[1], 1, left)
    total(1)
    send(tot_ref.at[1, :, down, :], got_ref.at[0], 2, right)
    total(3)
    send(tot_ref.at[3, :, up, :], got_ref.at[1], 3, left)
    total(0)
    copies[0].wait_recv()
    sum_ref[0] = hop_ref[0] + tot_ref[1, :, 0 : RHS // 2, :]
    send(sum_ref.at[0], got_ref.at[2], 4, right)
    copies[1].wait_recv()
    sum_ref[1] = hop_ref[1] + tot_ref[3, :, RHS // 2 : RHS, :]
    send(sum_ref.at[1], got_ref.at[3], 5, left)
    for k in (2, 3, 4, 5):
        copies[k].wait_recv()
    for ch in range(3):
        cols = slice(ch * 256, (ch + 1) * 256)
        y_ref[0 : RHS // 2, cols] = tot_ref[0, ch, 0 : RHS // 2, :] + got_ref[1, ch] + got_ref[2, ch]
        y_ref[RHS // 2 : RHS, cols] = tot_ref[0, ch, RHS // 2 : RHS, :] + got_ref[0, ch] + got_ref[3, ch]
    for cp in copies:
        cp.wait_send()


def cross_pairs(shift):
    pairs = []
    for c in range(2):
        for z in range(4):
            for y in range(4):
                for x in range(4):
                    z2 = (z + shift * c) % 4
                    y2 = (y + shift * (1 - c)) % 4
                    pairs.append((c * 64 + z * 16 + y * 4 + x, c * 64 + z2 * 16 + y2 * 4 + x))
    return pairs


VM = pl.BlockSpec(memory_space=pltpu.VMEM)
SM = pl.BlockSpec(memory_space=pltpu.SMEM)
FLOPS = 2 * ROWS * ROWS * (2 * FEAT + RHS) * NTGT


def solution(mesh):
    y_shape = jax.ShapeDtypeStruct((2, 5, 3, RHS, 256), F32)

    def product_call(kernel, consts, xt, args, blocks):
        return pl.pallas_call(
            kernel,
            out_shape=y_shape,
            in_specs=[SM] + [VM] * (1 + len(args)),
            out_specs=VM,
            scratch_shapes=[pltpu.VMEM((2, 3, 256, 256), BF), pltpu.VMEM((blocks, ROWS, 128), BF),
                            pltpu.VMEM((256, 256), BF)],
            compiler_params=pltpu.CompilerParams(vmem_limit_bytes=16 * 2**20),
            cost_estimate=pl.CostEstimate(flops=2 * FLOPS * blocks, bytes_accessed=2**20, transcendentals=0),
            name="product",
        )(consts, xt, *args)

    def local_rows(x_loc, v_loc, length_scale, out_scale):
        two_ell_sq = 2.0 * length_scale[0] * length_scale[0]
        consts = jnp.stack([(2.0 * LOG2E) / two_ell_sq, out_scale[0]])
        own, cross, line, xt = pl.pallas_call(
            gather_kernel,
            out_shape=(jax.ShapeDtypeStruct((1, SROWS, 128), BF), jax.ShapeDtypeStruct((2, SROWS, 128), BF),
                       jax.ShapeDtypeStruct((LINE, SROWS, 128), BF), jax.ShapeDtypeStruct((NTGT, GROUPS, 256, 128), BF)),
            in_specs=[SM, VM, VM],
            out_specs=(VM, VM, VM, VM),
            scratch_shapes=[pltpu.SemaphoreType.DMA((6,)), pltpu.SemaphoreType.DMA((LINE, 2)),
                            pltpu.SemaphoreType.DMA((2,)), pltpu.SemaphoreType.DMA((2,)),
                            pltpu.SemaphoreType.DMA((14,)), pltpu.SemaphoreType.DMA((NTGT, 2))],
            compiler_params=pltpu.CompilerParams(collective_id=0, has_side_effects=True, vmem_limit_bytes=16 * 2**20),
            name="gather",
        )(consts, x_loc, v_loc.T)
        up, down = [lax.ppermute(line, ("col", "row"), cross_pairs(d)) for d in (1, 3)]
        y1 = product_call(first_kernel, consts, xt, (own, cross, line), 6)
        y1, up, down, own, line = lax.optimization_barrier((y1, up, down, own, line))
        own, line = [lax.ppermute(a, ("col", "row"), cross_pairs(2)) for a in (own, line)]
        y2 = product_call(later_kernel, consts, xt, (y1, up, down), 6)
        y2, own, line = lax.optimization_barrier((y2, own, line))
        yp = product_call(later_kernel, consts, xt, (y2, own, line), 4)
        y_t = pl.pallas_call(
            reduce_kernel,
            out_shape=jax.ShapeDtypeStruct((RHS, ROWS), F32),
            in_specs=[VM],
            out_specs=VM,
            scratch_shapes=[pltpu.VMEM((4, 3, RHS, 256), F32), pltpu.VMEM((4, 3, RHS, 256), F32),
                            pltpu.VMEM((2, 3, RHS // 2, 256), F32), pltpu.VMEM((2, 3, RHS // 2, 256), F32),
                            pltpu.VMEM((4, 3, RHS // 2, 256), F32), pltpu.SemaphoreType.DMA((4,)),
                            pltpu.SemaphoreType.DMA((4,)), pltpu.SemaphoreType.DMA((6,)), pltpu.SemaphoreType.DMA((6,))],
            compiler_params=pltpu.CompilerParams(collective_id=1, has_side_effects=True, vmem_limit_bytes=8 * 2**20),
            name="reduce",
        )(yp)
        return y_t.T

    row_spec = P(("tasks", "row", "col"), None)
    rep_spec = P(None)
    return jax.shard_map(local_rows, mesh=mesh, in_specs=(row_spec, row_spec, rep_spec, rep_spec), out_specs=row_spec, check_vma=False)
```

```python
import functools

import jax
import jax.numpy as jnp
from jax import lax
from jax.experimental import pallas as pl
from jax.experimental.pallas import tpu as pltpu
from jax.sharding import PartitionSpec as P

BF = jnp.bfloat16
F32 = jnp.float32
ROWS = 768
FEAT = 128
RHS = 32
LINE = 4
NTGT = 8
GROUPS = 6
VROWS = GROUPS * RHS
NROWS = GROUPS * 16
NBASE = ROWS + VROWS
SROWS = ROWS + VROWS + NROWS
HALF = SROWS // 2
XROWS = 136
TILES = 3
PAIRS = 12
LOG2E = 1.4426950408889634
BIG = 3.0e38


def pieces(norm):
    half = jnp.maximum(norm * -0.5, -BIG)
    hi = half.astype(BF).astype(F32)
    rest = half - hi
    mid = rest.astype(BF).astype(F32)
    return hi, mid, rest - mid


def select(pos, at, vals):
    out = jnp.zeros_like(vals[0] + pos.astype(F32))
    for k, val in enumerate(vals):
        out = jnp.where(pos == at + k, val, out)
    return out


def position():
    col = lax.axis_index("col")
    row = lax.axis_index("row")
    return col, row // 16, (row // 4) % 4, row % 4


def device(col, z, y, x):
    return (0, col, (z % 4) * 16 + (y % 4) * 4 + x % 4)


def greet(peers):
    barrier = pltpu.get_barrier_semaphore()
    for peer in peers:
        pl.semaphore_signal(barrier, inc=1, device_id=peer, device_id_type=pl.DeviceIdType.MESH)


def enter(peers):
    pl.semaphore_wait(pltpu.get_barrier_semaphore(), len(peers))


def gather_kernel(sc_ref, x_ref, v_ref, sx_ref, xt_ref, v_buf, lsem, ssem, rsem, tsend, trecv):
    c, z, y, x = position()
    partner = device(1 - c, z, y, x)

    def along(d):
        return device(c, z + d * (1 - c), y + d * c, x)

    peers = [partner, along(1), along(3), device(c, z, y, x + 1), device(c, z, y, x + 3)]
    x_in = pltpu.make_async_copy(x_ref, sx_ref.at[0, pl.ds(0, ROWS), :], lsem.at[0])
    v_in = pltpu.make_async_copy(v_ref, v_buf, lsem.at[1])
    x_in.start()
    v_in.start()
    greet(peers)
    x_in.wait()
    xt = jnp.transpose(sx_ref[0, 0:ROWS, :].astype(F32))
    nrm = jnp.sum(xt * xt, axis=0, keepdims=True)
    hi, mid, low = pieces(nrm)
    pos = lax.broadcasted_iota(jnp.int32, (16, 128), 0)
    one = jnp.ones((1, 128), F32)
    parts = []
    for g in range(GROUPS):
        s = slice(g * 128, (g + 1) * 128)
        parts.append((hi[:, s], mid[:, s], low[:, s]))
        xt_ref[0, g, 0:FEAT, :] = xt[:, s].astype(BF)
        xt_ref[0, g, FEAT : FEAT + 16, :] = select(pos, 0, parts[g] + (one, one, one)).astype(BF)
    enter(peers)

    copies = []

    def src_part(slot, h):
        return sx_ref.at[slot, pl.ds(h * HALF, HALF), :]

    def send(src, dst, h, dev):
        cp = pltpu.make_async_remote_copy(src_part(src, h), src_part(dst, h), ssem.at[len(copies)], rsem.at[dst, h],
                                          device_id=dev, device_id_type=pl.DeviceIdType.MESH)
        cp.start()
        copies.append(cp)

    def got(slot, h):
        pltpu.make_async_remote_copy(src_part(slot, h), src_part(slot, h), ssem.at[0], rsem.at[slot, h],
                                     device_id=partner, device_id_type=pl.DeviceIdType.MESH).wait_recv()

    tcopies = []

    def tgt_part(slot, h):
        return xt_ref.at[slot, pl.ds(h * 3, 3), pl.ds(0, XROWS), :]

    def tsnd(src, dst, h, dev):
        cp = pltpu.make_async_remote_copy(tgt_part(src, h), tgt_part(dst, h), tsend.at[len(tcopies)], trecv.at[dst, h],
                                          device_id=dev, device_id_type=pl.DeviceIdType.MESH)
        cp.start()
        tcopies.append(cp)

    def tgot(slot, h):
        pltpu.make_async_remote_copy(tgt_part(slot, h), tgt_part(slot, h), tsend.at[0], trecv.at[slot, h],
                                     device_id=partner, device_id_type=pl.DeviceIdType.MESH).wait_recv()

    right = device(c, z, y, x + 1)
    left = device(c, z, y, x + 3)
    tsnd(0, 6, 0, right)
    tsnd(0, 2, 1, left)
    tsnd(0, 6, 1, right)
    tsnd(0, 2, 0, left)
    v_in.wait()
    for g in range(GROUPS):
        sx_ref[0, ROWS + g * RHS : ROWS + (g + 1) * RHS, :] = v_buf[:, g * 128 : (g + 1) * 128]
        sx_ref[0, NBASE + g * 16 : NBASE + (g + 1) * 16, :] = select(pos, 0, (one, one, one) + parts[g]).astype(BF)
    send(0, 3, 0, along(1))
    send(0, 1, 1, along(3))
    send(0, 3, 1, along(1))
    send(0, 1, 0, along(3))
    for h in range(2):
        tsnd(0, 1, h, partner)
    for t in range(NTGT):
        for g in range(GROUPS):
            xt_ref[t, g, FEAT + 16 : 256, :] = jnp.zeros((112, 128), BF)
            if t:
                xt_ref[t, g, XROWS : FEAT + 16, :] = jnp.zeros((FEAT + 16 - XROWS, 128), BF)
    got(3, 0)
    send(3, 2, 0, along(1))
    got(1, 1)
    send(1, 2, 1, along(3))
    tgot(6, 0)
    tsnd(6, 4, 0, right)
    tgot(2, 1)
    tsnd(2, 4, 1, left)
    tsnd(6, 7, 0, partner)
    tsnd(2, 3, 1, partner)
    tgot(6, 1)
    tsnd(6, 7, 1, partner)
    tgot(2, 0)
    tsnd(2, 3, 0, partner)
    got(3, 1)
    got(1, 0)
    got(2, 0)
    got(2, 1)
    for h in range(2):
        tgot(4, h)
        tsnd(4, 5, h, partner)
    for t in (1, 3, 7, 5):
        for h in range(2):
            tgot(t, h)
    for cp in copies:
        cp.wait_send()
    for cp in tcopies:
        cp.wait_send()


def product(alpha, scale, srcs, xt_ref, y_ref, tile_ref, aug_ref, eye_ref):
    piece = 64
    n_pc = 256 // piece
    per_pair = len(srcs) * TILES
    span = 48 // per_pair
    steps = span * per_pair

    def run(*accs):
        per = 3 * n_pc + span + 1
        gram = [[[accs[q * per + r * n_pc + p] for p in range(n_pc)] for r in range(3)] for q in range(2)]
        body_acc = [[accs[q * per + 3 * n_pc + w] for q in range(2)] for w in range(span)]
        tail_acc = [accs[q * per + 3 * n_pc + span] for q in range(2)]

        def acc_gram(q, u, t, p):
            rows = pl.ds((t % TILES) * 256 + p * piece, piece)
            lhs = jnp.concatenate([srcs[t // TILES][rows, :], aug_ref[t // TILES, rows, :]], axis=1)
            pltpu.matmul_acc_lhs(gram[q][u % 3][p], lhs, load_staged_rhs=0 if p == 0 else None)

        def push_x(q, pair):
            tgt = (pair // 3) * 2 + q
            ch = (pair % 3) * 2
            pltpu.matmul_push_rhs(jnp.concatenate([xt_ref[tgt, ch], xt_ref[tgt, ch + 1]], axis=1),
                                  staging_register=0, mxu_index=q)

        def push_tile(q, u):
            pltpu.matmul_push_rhs(tile_ref[q, (u - 1) % 3], staging_register=1, mxu_index=q)

        def values(q, u, p):
            half = pltpu.matmul_pop(gram[q][(u - 2) % 3][p])
            kern = (jnp.exp2(jnp.minimum(half * alpha, 0.0)) * scale).astype(BF)
            tile_ref[q, u % 3, p * piece : (p + 1) * piece, :] = kern

        def acc_y(q, t, acc):
            lo = ROWS + (t % TILES) * 2 * RHS
            src = srcs[t // TILES]
            vt = jnp.concatenate([src[pl.ds(lo, RHS), :], src[pl.ds(lo + RHS, RHS), :]], axis=1)
            pltpu.matmul_acc_lhs(acc[q], vt, load_staged_rhs=1)

        def add_y(acc, pair):
            for q in range(2):
                y_ref[q, pair // 3, pair % 3] += pltpu.matmul_pop(acc[q])

        def clear():
            for q in range(2):
                for r in range(3):
                    for p in range(n_pc):
                        pltpu.matmul_pop(gram[q][r][p])
                for acc in body_acc:
                    pltpu.matmul_pop(acc[q])
                pltpu.matmul_pop(tail_acc[q])

        def norm_columns():
            row = lax.broadcasted_iota(jnp.int32, (256, 256), 0)
            colm = lax.broadcasted_iota(jnp.int32, (256, 256), 1)
            eye_ref[...] = jnp.where(row == colm, 1.0, 0.0).astype(BF)

            def take(n):
                for p in range(n_pc):
                    cols = pltpu.matmul_pop(gram[n % 2][(n // 2) % 3][p])
                    for h in range(2):
                        i = 2 * n + h
                        rows = pl.ds((i % TILES) * 256 + p * piece, piece)
                        aug_ref[i // TILES, rows, :] = cols[:, h * 128 : (h + 1) * 128].astype(BF)

            blank = jnp.zeros((112, 256), BF)
            count = per_pair // 2
            for n in range(count):
                rows = []
                for i in (2 * n, 2 * n + 1):
                    src = srcs[i // TILES]
                    lo = NBASE + (i % TILES) * 32
                    rows += [jnp.concatenate([src[pl.ds(lo, 16), :], src[pl.ds(lo + 16, 16), :]], axis=1), blank]
                pltpu.matmul_push_rhs(jnp.concatenate(rows, axis=0), staging_register=0, mxu_index=n % 2, transpose=True)
                for p in range(n_pc):
                    pltpu.matmul_acc_lhs(gram[n % 2][(n // 2) % 3][p], eye_ref[p * piece : (p + 1) * piece, :],
                                         load_staged_rhs=0 if p == 0 else None)
                if n >= 4:
                    take(n - 4)
            for n in range(count - 4, count):
                take(n)

        def trip(k, carry):
            old = jnp.where(k == 0, PAIRS, k * span - 1)
            for u in range(steps):
                if u < steps - 1:
                    nxt = k * span + (u + 1) // per_pair
                else:
                    nxt = jnp.minimum((k + 1) * span, PAIRS - 1)
                for q in range(2):
                    push_tile(q, u)
                for p in range(n_pc):
                    for q in range(2):
                        acc_gram(q, u, u % per_pair, p)
                        if p == 0:
                            push_x(q, nxt)
                    for q in range(2):
                        values(q, u, p)
                for q in range(2):
                    if u < 3:
                        acc_y(q, per_pair - 3 + u, tail_acc)
                    else:
                        acc_y(q, (u - 3) % per_pair, body_acc[(u - 3) // per_pair])
                if u == 1:
                    add_y(body_acc[span - 1], old)
                if u == 6:
                    add_y(tail_acc, old)
                for w in range(span - 1):
                    if u == (w + 1) * per_pair + 8:
                        add_y(body_acc[w], k * span + w)
            return carry

        clear()
        norm_columns()
        for q in range(2):
            push_x(q, 0)
        lax.fori_loop(0, PAIRS // span, trip, 0)
        for u in range(steps, steps + 3):
            for q in range(2):
                push_tile(q, u)
                if u < steps + 2:
                    for p in range(n_pc):
                        values(q, u, p)
                acc_y(q, (u - 3) % per_pair, tail_acc)
        add_y(body_acc[span - 1], PAIRS - 1)
        for q in range(2):
            acc_gram(q, 0, 0, 0)
            pltpu.matmul_pop(gram[q][0][0])
        add_y(tail_acc, PAIRS - 1)

    specs = []
    for q in range(2):
        specs += [pltpu.ACC(q)((piece, 256), F32)] * (3 * n_pc) + [pltpu.ACC(q)((RHS, 256), F32)] * (span + 1)
    pl.run_scoped(run, *specs)


def first_kernel(sc_ref, xt_ref, src_ref, y_ref, tile_ref, aug_ref, eye_ref):
    y_ref[...] = jnp.zeros_like(y_ref)
    srcs = [src_ref.at[b] for b in range(LINE)]
    product(sc_ref[0], sc_ref[1], srcs, xt_ref, y_ref, tile_ref, aug_ref, eye_ref)


def later_kernel(sc_ref, xt_ref, yin_ref, *refs):
    y_ref, tile_ref, aug_ref, eye_ref = refs[-4:]
    y_ref[...] = yin_ref[...]
    srcs = [ref.at[b] for ref in refs[:-4] for b in range(LINE)]
    product(sc_ref[0], sc_ref[1], srcs, xt_ref, y_ref, tile_ref, aug_ref, eye_ref)


def reduce_kernel(yp_ref, y_ref, part_ref, tot_ref, hop_ref, sum_ref, got_ref, psend, precv, ssem, rsem):
    c, z, y, x = position()
    partner = device(1 - c, z, y, x)
    right = device(c, z, y, x + 1)
    left = device(c, z, y, x + 3)
    peers = [partner, right, left]
    greet(peers)
    enter(peers)
    up = pl.ds(0, RHS // 2)
    down = pl.ds(RHS // 2, RHS // 2)
    copies = []

    def send(src, dst, k, dev):
        cp = pltpu.make_async_remote_copy(src, dst, ssem.at[k], rsem.at[k], device_id=dev,
                                          device_id_type=pl.DeviceIdType.MESH)
        cp.start()
        copies.append(cp)

    first = {}
    for d in (2, 1, 3, 0):
        first[d] = pltpu.make_async_remote_copy(yp_ref.at[1, d], part_ref.at[d], psend.at[d], precv.at[d],
                                                device_id=partner, device_id_type=pl.DeviceIdType.MESH)
        first[d].start()

    def total(d):
        first[d].wait()
        tot_ref[d] = yp_ref[0, d] + part_ref[d]

    total(2)
    send(tot_ref.at[2, :, up, :], hop_ref.at[0], 0, right)
    send(tot_ref.at[2, :, down, :], hop_ref.at[1], 1, left)
    total(1)
    send(tot_ref.at[1, :, down, :], got_ref.at[0], 2, right)
    total(3)
    send(tot_ref.at[3, :, up, :], got_ref.at[1], 3, left)
    total(0)
    copies[0].wait_recv()
    sum_ref[0] = hop_ref[0] + tot_ref[1, :, 0 : RHS // 2, :]
    send(sum_ref.at[0], got_ref.at[2], 4, right)
    copies[1].wait_recv()
    sum_ref[1] = hop_ref[1] + tot_ref[3, :, RHS // 2 : RHS, :]
    send(sum_ref.at[1], got_ref.at[3], 5, left)
    for k in (2, 3, 4, 5):
        copies[k].wait_recv()
    for ch in range(3):
        cols = slice(ch * 256, (ch + 1) * 256)
        y_ref[0 : RHS // 2, cols] = tot_ref[0, ch, 0 : RHS // 2, :] + got_ref[1, ch] + got_ref[2, ch]
        y_ref[RHS // 2 : RHS, cols] = tot_ref[0, ch, RHS // 2 : RHS, :] + got_ref[0, ch] + got_ref[3, ch]
    for cp in copies:
        cp.wait_send()


def cross_pairs(shift):
    pairs = []
    for c in range(2):
        for z in range(4):
            for y in range(4):
                for x in range(4):
                    z2 = (z + shift * c) % 4
                    y2 = (y + shift * (1 - c)) % 4
                    pairs.append((c * 64 + z * 16 + y * 4 + x, c * 64 + z2 * 16 + y2 * 4 + x))
    return pairs


VM = pl.BlockSpec(memory_space=pltpu.VMEM)
ANY = pl.BlockSpec(memory_space=pltpu.HBM)
SM = pl.BlockSpec(memory_space=pltpu.SMEM)
FLOPS = 2 * ROWS * ROWS * (2 * FEAT + RHS) * NTGT


def solution(mesh):
    y_shape = jax.ShapeDtypeStruct((2, 5, 3, RHS, 256), F32)

    def product_call(kernel, consts, xt, args, lines):
        return pl.pallas_call(
            kernel,
            out_shape=y_shape,
            in_specs=[SM] + [VM] * (1 + len(args)),
            out_specs=VM,
            scratch_shapes=[pltpu.VMEM((2, 3, 256, 256), BF), pltpu.VMEM((lines * LINE, ROWS, 128), BF),
                            pltpu.VMEM((256, 256), BF)],
            compiler_params=pltpu.CompilerParams(vmem_limit_bytes=16 * 2**20),
            cost_estimate=pl.CostEstimate(flops=2 * FLOPS * LINE * lines, bytes_accessed=2**20, transcendentals=0),
            name="product",
        )(consts, xt, *args)

    def local_rows(x_loc, v_loc, length_scale, out_scale):
        two_ell_sq = 2.0 * length_scale[0] * length_scale[0]
        consts = jnp.stack([(2.0 * LOG2E) / two_ell_sq, out_scale[0]])
        line, xt = pl.pallas_call(
            gather_kernel,
            out_shape=(jax.ShapeDtypeStruct((LINE, SROWS, 128), BF), jax.ShapeDtypeStruct((NTGT, GROUPS, 256, 128), BF)),
            in_specs=[SM, ANY, ANY],
            out_specs=(VM, VM),
            scratch_shapes=[pltpu.VMEM((RHS, ROWS), BF), pltpu.SemaphoreType.DMA((2,)),
                            pltpu.SemaphoreType.DMA((6,)), pltpu.SemaphoreType.DMA((LINE, 2)),
                            pltpu.SemaphoreType.DMA((14,)), pltpu.SemaphoreType.DMA((NTGT, 2))],
            compiler_params=pltpu.CompilerParams(collective_id=0, has_side_effects=True, vmem_limit_bytes=16 * 2**20),
            name="gather",
        )(consts, pltpu.with_memory_space_constraint(x_loc, pltpu.HBM), pltpu.with_memory_space_constraint(v_loc.T, pltpu.HBM))
        up, down = [lax.ppermute(line, ("col", "row"), cross_pairs(d)) for d in (1, 3)]
        y1 = product_call(first_kernel, consts, xt, (line,), 1)
        y1, up, down, line = lax.optimization_barrier((y1, up, down, line))
        across = lax.ppermute(line, ("col", "row"), cross_pairs(2))
        y2 = product_call(later_kernel, consts, xt, (y1, up, down), 2)
        y2, across = lax.optimization_barrier((y2, across))
        yp = product_call(later_kernel, consts, xt, (y2, across), 1)
        y_t = pl.pallas_call(
            reduce_kernel,
            out_shape=jax.ShapeDtypeStruct((RHS, ROWS), F32),
            in_specs=[VM],
            out_specs=VM,
            scratch_shapes=[pltpu.VMEM((4, 3, RHS, 256), F32), pltpu.VMEM((4, 3, RHS, 256), F32),
                            pltpu.VMEM((2, 3, RHS // 2, 256), F32), pltpu.VMEM((2, 3, RHS // 2, 256), F32),
                            pltpu.VMEM((4, 3, RHS // 2, 256), F32), pltpu.SemaphoreType.DMA((4,)),
                            pltpu.SemaphoreType.DMA((4,)), pltpu.SemaphoreType.DMA((6,)), pltpu.SemaphoreType.DMA((6,))],
            compiler_params=pltpu.CompilerParams(collective_id=1, has_side_effects=True, vmem_limit_bytes=8 * 2**20),
            name="reduce",
        )(yp)
        return y_t.T

    row_spec = P(("tasks", "row", "col"), None)
    rep_spec = P(None)
    return jax.shard_map(local_rows, mesh=mesh, in_specs=(row_spec, row_spec, rep_spec, rep_spec), out_specs=row_spec, check_vma=False)
```

```python
import functools

import jax
import jax.numpy as jnp
from jax import lax
from jax.experimental import pallas as pl
from jax.experimental.pallas import tpu as pltpu
from jax.sharding import PartitionSpec as P

BF = jnp.bfloat16
F32 = jnp.float32
ROWS = 768
FEAT = 128
RHS = 32
LINE = 4
NTGT = 8
GROUPS = 6
VROWS = GROUPS * RHS
NROWS = GROUPS * 16
NBASE = ROWS + VROWS
SROWS = ROWS + VROWS + NROWS
HALF = SROWS // 2
XROWS = 136
TILES = 3
PAIRS = 12
LOG2E = 1.4426950408889634
BIG = 3.0e38


def pieces(norm):
    half = jnp.maximum(norm * -0.5, -BIG)
    hi = half.astype(BF).astype(F32)
    rest = half - hi
    mid = rest.astype(BF).astype(F32)
    return hi, mid, rest - mid


def select(pos, at, vals):
    out = jnp.zeros_like(vals[0] + pos.astype(F32))
    for k, val in enumerate(vals):
        out = jnp.where(pos == at + k, val, out)
    return out


def position():
    col = lax.axis_index("col")
    row = lax.axis_index("row")
    return col, row // 16, (row // 4) % 4, row % 4


def device(col, z, y, x):
    return (0, col, (z % 4) * 16 + (y % 4) * 4 + x % 4)


def greet(peers):
    barrier = pltpu.get_barrier_semaphore()
    for peer in peers:
        pl.semaphore_signal(barrier, inc=1, device_id=peer, device_id_type=pl.DeviceIdType.MESH)


def enter(peers):
    pl.semaphore_wait(pltpu.get_barrier_semaphore(), len(peers))


def gather_kernel(sc_ref, x_ref, v_ref, sx_ref, xt_ref, v_buf, lsem, ssem, rsem, tsend, trecv):
    c, z, y, x = position()
    partner = device(1 - c, z, y, x)

    def along(d):
        return device(c, z + d * (1 - c), y + d * c, x)

    peers = [partner, along(1), along(3), device(c, z, y, x + 1), device(c, z, y, x + 3)]
    x_in = pltpu.make_async_copy(x_ref, sx_ref.at[0, pl.ds(0, ROWS), :], lsem.at[0])
    v_in = pltpu.make_async_copy(v_ref, v_buf, lsem.at[1])
    x_in.start()
    v_in.start()
    greet(peers)
    x_in.wait()
    xt = jnp.transpose(sx_ref[0, 0:ROWS, :].astype(F32))
    nrm = jnp.sum(xt * xt, axis=0, keepdims=True)
    hi, mid, low = pieces(nrm)
    pos = lax.broadcasted_iota(jnp.int32, (16, 128), 0)
    one = jnp.ones((1, 128), F32)
    parts = []
    for g in range(GROUPS):
        s = slice(g * 128, (g + 1) * 128)
        parts.append((hi[:, s], mid[:, s], low[:, s]))
        xt_ref[0, g, 0:FEAT, :] = xt[:, s].astype(BF)
        xt_ref[0, g, FEAT : FEAT + 16, :] = select(pos, 0, parts[g] + (one, one, one)).astype(BF)
    enter(peers)

    copies = []

    def src_part(slot, h):
        return sx_ref.at[slot, pl.ds(h * HALF, HALF), :]

    def send(src, dst, h, dev):
        cp = pltpu.make_async_remote_copy(src_part(src, h), src_part(dst, h), ssem.at[len(copies)], rsem.at[dst, h],
                                          device_id=dev, device_id_type=pl.DeviceIdType.MESH)
        cp.start()
        copies.append(cp)

    def got(slot, h):
        pltpu.make_async_remote_copy(src_part(slot, h), src_part(slot, h), ssem.at[0], rsem.at[slot, h],
                                     device_id=partner, device_id_type=pl.DeviceIdType.MESH).wait_recv()

    tcopies = []

    def tgt_part(slot, h):
        return xt_ref.at[slot, pl.ds(h * 3, 3), pl.ds(0, XROWS), :]

    def tsnd(src, dst, h, dev):
        cp = pltpu.make_async_remote_copy(tgt_part(src, h), tgt_part(dst, h), tsend.at[len(tcopies)], trecv.at[dst, h],
                                          device_id=dev, device_id_type=pl.DeviceIdType.MESH)
        cp.start()
        tcopies.append(cp)

    def tgot(slot, h):
        pltpu.make_async_remote_copy(tgt_part(slot, h), tgt_part(slot, h), tsend.at[0], trecv.at[slot, h],
                                     device_id=partner, device_id_type=pl.DeviceIdType.MESH).wait_recv()

    right = device(c, z, y, x + 1)
    left = device(c, z, y, x + 3)
    tsnd(0, 6, 0, right)
    tsnd(0, 2, 1, left)
    tsnd(0, 6, 1, right)
    tsnd(0, 2, 0, left)
    v_in.wait()
    for g in range(GROUPS):
        sx_ref[0, ROWS + g * RHS : ROWS + (g + 1) * RHS, :] = v_buf[:, g * 128 : (g + 1) * 128]
        sx_ref[0, NBASE + g * 16 : NBASE + (g + 1) * 16, :] = select(pos, 0, (one, one, one) + parts[g]).astype(BF)
    send(0, 3, 0, along(1))
    send(0, 1, 1, along(3))
    send(0, 3, 1, along(1))
    send(0, 1, 0, along(3))
    for h in range(2):
        tsnd(0, 1, h, partner)
    for t in range(NTGT):
        for g in range(GROUPS):
            xt_ref[t, g, FEAT + 16 : 256, :] = jnp.zeros((112, 128), BF)
            if t:
                xt_ref[t, g, XROWS : FEAT + 16, :] = jnp.zeros((FEAT + 16 - XROWS, 128), BF)
    got(3, 0)
    send(3, 2, 0, along(1))
    got(1, 1)
    send(1, 2, 1, along(3))
    tgot(6, 0)
    tsnd(6, 4, 0, right)
    tgot(2, 1)
    tsnd(2, 4, 1, left)
    tsnd(6, 7, 0, partner)
    tsnd(2, 3, 1, partner)
    tgot(6, 1)
    tsnd(6, 7, 1, partner)
    tgot(2, 0)
    tsnd(2, 3, 0, partner)
    got(3, 1)
    got(1, 0)
    got(2, 0)
    got(2, 1)
    for h in range(2):
        tgot(4, h)
        tsnd(4, 5, h, partner)
    for t in (1, 3, 7, 5):
        for h in range(2):
            tgot(t, h)
    for cp in copies:
        cp.wait_send()
    for cp in tcopies:
        cp.wait_send()


def product(sc_ref, srcs, xt_ref, y_ref, tile_ref, aug_ref, eye_ref):
    alpha = jnp.concatenate([sc_ref[0:1, :], sc_ref[0:1, :]], axis=1)
    scale = jnp.concatenate([sc_ref[1:2, :], sc_ref[1:2, :]], axis=1)
    piece = 64
    n_pc = 256 // piece
    per_pair = len(srcs) * TILES
    span = 48 // per_pair
    steps = span * per_pair

    def run(*accs):
        per = 3 * n_pc + span + 1
        gram = [[[accs[q * per + r * n_pc + p] for p in range(n_pc)] for r in range(3)] for q in range(2)]
        body_acc = [[accs[q * per + 3 * n_pc + w] for q in range(2)] for w in range(span)]
        tail_acc = [accs[q * per + 3 * n_pc + span] for q in range(2)]

        def acc_gram(q, u, t, p):
            rows = pl.ds((t % TILES) * 256 + p * piece, piece)
            lhs = jnp.concatenate([srcs[t // TILES][rows, :], aug_ref[t // TILES, rows, :]], axis=1)
            pltpu.matmul_acc_lhs(gram[q][u % 3][p], lhs, load_staged_rhs=0 if p == 0 else None)

        def push_x(q, pair):
            tgt = (pair // 3) * 2 + q
            ch = (pair % 3) * 2
            pltpu.matmul_push_rhs(jnp.concatenate([xt_ref[tgt, ch], xt_ref[tgt, ch + 1]], axis=1),
                                  staging_register=0, mxu_index=q)

        def push_tile(q, u):
            pltpu.matmul_push_rhs(tile_ref[q, (u - 1) % 3], staging_register=1, mxu_index=q)

        def values(q, u, p):
            half = pltpu.matmul_pop(gram[q][(u - 2) % 3][p])
            kern = (jnp.exp2(jnp.minimum(half * alpha, 0.0)) * scale).astype(BF)
            tile_ref[q, u % 3, p * piece : (p + 1) * piece, :] = kern

        def acc_y(q, t, acc):
            lo = ROWS + (t % TILES) * 2 * RHS
            src = srcs[t // TILES]
            vt = jnp.concatenate([src[pl.ds(lo, RHS), :], src[pl.ds(lo + RHS, RHS), :]], axis=1)
            pltpu.matmul_acc_lhs(acc[q], vt, load_staged_rhs=1)

        def add_y(acc, pair):
            for q in range(2):
                y_ref[q, pair // 3, pair % 3] += pltpu.matmul_pop(acc[q])

        def clear():
            for q in range(2):
                for r in range(3):
                    for p in range(n_pc):
                        pltpu.matmul_pop(gram[q][r][p])
                for acc in body_acc:
                    pltpu.matmul_pop(acc[q])
                pltpu.matmul_pop(tail_acc[q])

        def norm_columns():
            row = lax.broadcasted_iota(jnp.int32, (256, 256), 0)
            colm = lax.broadcasted_iota(jnp.int32, (256, 256), 1)
            eye_ref[...] = jnp.where(row == colm, 1.0, 0.0).astype(BF)

            def take(n):
                for p in range(n_pc):
                    cols = pltpu.matmul_pop(gram[n % 2][(n // 2) % 3][p])
                    for h in range(2):
                        i = 2 * n + h
                        rows = pl.ds((i % TILES) * 256 + p * piece, piece)
                        aug_ref[i // TILES, rows, :] = cols[:, h * 128 : (h + 1) * 128].astype(BF)

            blank = jnp.zeros((112, 256), BF)
            count = per_pair // 2
            for n in range(count):
                rows = []
                for i in (2 * n, 2 * n + 1):
                    src = srcs[i // TILES]
                    lo = NBASE + (i % TILES) * 32
                    rows += [jnp.concatenate([src[pl.ds(lo, 16), :], src[pl.ds(lo + 16, 16), :]], axis=1), blank]
                pltpu.matmul_push_rhs(jnp.concatenate(rows, axis=0), staging_register=0, mxu_index=n % 2, transpose=True)
                for p in range(n_pc):
                    pltpu.matmul_acc_lhs(gram[n % 2][(n // 2) % 3][p], eye_ref[p * piece : (p + 1) * piece, :],
                                         load_staged_rhs=0 if p == 0 else None)
                if n >= 4:
                    take(n - 4)
            for n in range(count - 4, count):
                take(n)

        def trip(k, carry):
            old = jnp.where(k == 0, PAIRS, k * span - 1)
            for u in range(steps):
                if u < steps - 1:
                    nxt = k * span + (u + 1) // per_pair
                else:
                    nxt = jnp.minimum((k + 1) * span, PAIRS - 1)
                for q in range(2):
                    push_tile(q, u)
                for p in range(n_pc):
                    for q in range(2):
                        acc_gram(q, u, u % per_pair, p)
                        if p == 0:
                            push_x(q, nxt)
                    for q in range(2):
                        values(q, u, p)
                for q in range(2):
                    if u < 3:
                        acc_y(q, per_pair - 3 + u, tail_acc)
                    else:
                        acc_y(q, (u - 3) % per_pair, body_acc[(u - 3) // per_pair])
                if u == 1:
                    add_y(body_acc[span - 1], old)
                if u == 6:
                    add_y(tail_acc, old)
                for w in range(span - 1):
                    if u == (w + 1) * per_pair + 8:
                        add_y(body_acc[w], k * span + w)
            return carry

        clear()
        norm_columns()
        for q in range(2):
            push_x(q, 0)
        lax.fori_loop(0, PAIRS // span, trip, 0)
        for u in range(steps, steps + 3):
            for q in range(2):
                push_tile(q, u)
                if u < steps + 2:
                    for p in range(n_pc):
                        values(q, u, p)
                acc_y(q, (u - 3) % per_pair, tail_acc)
        add_y(body_acc[span - 1], PAIRS - 1)
        for q in range(2):
            acc_gram(q, 0, 0, 0)
            pltpu.matmul_pop(gram[q][0][0])
        add_y(tail_acc, PAIRS - 1)

    specs = []
    for q in range(2):
        specs += [pltpu.ACC(q)((piece, 256), F32)] * (3 * n_pc) + [pltpu.ACC(q)((RHS, 256), F32)] * (span + 1)
    pl.run_scoped(run, *specs)


def first_kernel(sc_ref, xt_ref, src_ref, y_ref, tile_ref, aug_ref, eye_ref):
    y_ref[...] = jnp.zeros_like(y_ref)
    srcs = [src_ref.at[b] for b in range(LINE)]
    product(sc_ref, srcs, xt_ref, y_ref, tile_ref, aug_ref, eye_ref)


def later_kernel(sc_ref, xt_ref, yin_ref, *refs):
    y_ref, tile_ref, aug_ref, eye_ref = refs[-4:]
    y_ref[...] = yin_ref[...]
    srcs = [ref.at[b] for ref in refs[:-4] for b in range(LINE)]
    product(sc_ref, srcs, xt_ref, y_ref, tile_ref, aug_ref, eye_ref)


def reduce_kernel(yp_ref, y_ref, part_ref, tot_ref, hop_ref, sum_ref, got_ref, psend, precv, ssem, rsem):
    c, z, y, x = position()
    partner = device(1 - c, z, y, x)
    right = device(c, z, y, x + 1)
    left = device(c, z, y, x + 3)
    peers = [partner, right, left]
    greet(peers)
    enter(peers)
    up = pl.ds(0, RHS // 2)
    down = pl.ds(RHS // 2, RHS // 2)
    copies = []

    def send(src, dst, k, dev):
        cp = pltpu.make_async_remote_copy(src, dst, ssem.at[k], rsem.at[k], device_id=dev,
                                          device_id_type=pl.DeviceIdType.MESH)
        cp.start()
        copies.append(cp)

    first = {}
    for d in (2, 1, 3, 0):
        first[d] = pltpu.make_async_remote_copy(yp_ref.at[1, d], part_ref.at[d], psend.at[d], precv.at[d],
                                                device_id=partner, device_id_type=pl.DeviceIdType.MESH)
        first[d].start()

    def total(d):
        first[d].wait()
        tot_ref[d] = yp_ref[0, d] + part_ref[d]

    total(2)
    send(tot_ref.at[2, :, up, :], hop_ref.at[0], 0, right)
    send(tot_ref.at[2, :, down, :], hop_ref.at[1], 1, left)
    total(1)
    send(tot_ref.at[1, :, down, :], got_ref.at[0], 2, right)
    total(3)
    send(tot_ref.at[3, :, up, :], got_ref.at[1], 3, left)
    total(0)
    copies[0].wait_recv()
    sum_ref[0] = hop_ref[0] + tot_ref[1, :, 0 : RHS // 2, :]
    send(sum_ref.at[0], got_ref.at[2], 4, right)
    copies[1].wait_recv()
    sum_ref[1] = hop_ref[1] + tot_ref[3, :, RHS // 2 : RHS, :]
    send(sum_ref.at[1], got_ref.at[3], 5, left)
    for k in (2, 3, 4, 5):
        copies[k].wait_recv()
    for ch in range(3):
        cols = slice(ch * 256, (ch + 1) * 256)
        y_ref[0 : RHS // 2, cols] = tot_ref[0, ch, 0 : RHS // 2, :] + got_ref[1, ch] + got_ref[2, ch]
        y_ref[RHS // 2 : RHS, cols] = tot_ref[0, ch, RHS // 2 : RHS, :] + got_ref[0, ch] + got_ref[3, ch]
    for cp in copies:
        cp.wait_send()


def cross_pairs(shift):
    pairs = []
    for c in range(2):
        for z in range(4):
            for y in range(4):
                for x in range(4):
                    z2 = (z + shift * c) % 4
                    y2 = (y + shift * (1 - c)) % 4
                    pairs.append((c * 64 + z * 16 + y * 4 + x, c * 64 + z2 * 16 + y2 * 4 + x))
    return pairs


VM = pl.BlockSpec(memory_space=pltpu.VMEM)
ANY = pl.BlockSpec(memory_space=pltpu.HBM)
FLOPS = 2 * ROWS * ROWS * (2 * FEAT + RHS) * NTGT


def solution(mesh):
    y_shape = jax.ShapeDtypeStruct((2, 5, 3, RHS, 256), F32)

    def product_call(kernel, consts, xt, args, lines):
        return pl.pallas_call(
            kernel,
            out_shape=y_shape,
            in_specs=[VM] + [VM] * (1 + len(args)),
            out_specs=VM,
            scratch_shapes=[pltpu.VMEM((2, 3, 256, 256), BF), pltpu.VMEM((lines * LINE, ROWS, 128), BF),
                            pltpu.VMEM((256, 256), BF)],
            compiler_params=pltpu.CompilerParams(vmem_limit_bytes=16 * 2**20),
            cost_estimate=pl.CostEstimate(flops=2 * FLOPS * LINE * lines, bytes_accessed=2**20, transcendentals=0),
            name="product",
        )(consts, xt, *args)

    def local_rows(x_loc, v_loc, length_scale, out_scale):
        two_ell_sq = 2.0 * length_scale[0] * length_scale[0]
        consts = jnp.broadcast_to(jnp.stack([(2.0 * LOG2E) / two_ell_sq, out_scale[0]])[:, None], (2, 128))
        line, xt = pl.pallas_call(
            gather_kernel,
            out_shape=(jax.ShapeDtypeStruct((LINE, SROWS, 128), BF), jax.ShapeDtypeStruct((NTGT, GROUPS, 256, 128), BF)),
            in_specs=[ANY, ANY, ANY],
            out_specs=(VM, VM),
            scratch_shapes=[pltpu.VMEM((RHS, ROWS), BF), pltpu.SemaphoreType.DMA((2,)),
                            pltpu.SemaphoreType.DMA((6,)), pltpu.SemaphoreType.DMA((LINE, 2)),
                            pltpu.SemaphoreType.DMA((14,)), pltpu.SemaphoreType.DMA((NTGT, 2))],
            compiler_params=pltpu.CompilerParams(collective_id=0, has_side_effects=True, vmem_limit_bytes=16 * 2**20),
            name="gather",
        )(consts, pltpu.with_memory_space_constraint(x_loc, pltpu.HBM), pltpu.with_memory_space_constraint(v_loc.T, pltpu.HBM))
        up, down = [lax.ppermute(line, ("col", "row"), cross_pairs(d)) for d in (1, 3)]
        y1 = product_call(first_kernel, consts, xt, (line,), 1)
        y1, up, down, line = lax.optimization_barrier((y1, up, down, line))
        across = lax.ppermute(line, ("col", "row"), cross_pairs(2))
        y2 = product_call(later_kernel, consts, xt, (y1, up, down), 2)
        y2, across = lax.optimization_barrier((y2, across))
        yp = product_call(later_kernel, consts, xt, (y2, across), 1)
        y_t = pl.pallas_call(
            reduce_kernel,
            out_shape=jax.ShapeDtypeStruct((RHS, ROWS), F32),
            in_specs=[VM],
            out_specs=VM,
            scratch_shapes=[pltpu.VMEM((4, 3, RHS, 256), F32), pltpu.VMEM((4, 3, RHS, 256), F32),
                            pltpu.VMEM((2, 3, RHS // 2, 256), F32), pltpu.VMEM((2, 3, RHS // 2, 256), F32),
                            pltpu.VMEM((4, 3, RHS // 2, 256), F32), pltpu.SemaphoreType.DMA((4,)),
                            pltpu.SemaphoreType.DMA((4,)), pltpu.SemaphoreType.DMA((6,)), pltpu.SemaphoreType.DMA((6,))],
            compiler_params=pltpu.CompilerParams(collective_id=1, has_side_effects=True, vmem_limit_bytes=8 * 2**20),
            name="reduce",
        )(yp)
        return y_t.T

    row_spec = P(("tasks", "row", "col"), None)
    rep_spec = P(None)
    return jax.shard_map(local_rows, mesh=mesh, in_specs=(row_spec, row_spec, rep_spec, rep_spec), out_specs=row_spec, check_vma=False)
```

```python
import functools

import jax
import jax.numpy as jnp
from jax import lax
from jax.experimental import pallas as pl
from jax.experimental.pallas import tpu as pltpu
from jax.sharding import PartitionSpec as P

BF = jnp.bfloat16
F32 = jnp.float32
ROWS = 768
FEAT = 128
RHS = 32
LINE = 4
NTGT = 8
GROUPS = 6
VROWS = GROUPS * RHS
NROWS = GROUPS * 16
NBASE = ROWS + VROWS
SROWS = ROWS + VROWS + NROWS
HALF = SROWS // 2
XROWS = 136
TILES = 3
PAIRS = 12
LOG2E = 1.4426950408889634
BIG = 3.0e38


def pieces(norm):
    half = jnp.maximum(norm * -0.5, -BIG)
    hi = half.astype(BF).astype(F32)
    rest = half - hi
    mid = rest.astype(BF).astype(F32)
    return hi, mid, rest - mid


def select(pos, at, vals):
    out = jnp.zeros_like(vals[0] + pos.astype(F32))
    for k, val in enumerate(vals):
        out = jnp.where(pos == at + k, val, out)
    return out


def position():
    col = lax.axis_index("col")
    row = lax.axis_index("row")
    return col, row // 16, (row // 4) % 4, row % 4


def device(col, z, y, x):
    return (0, col, (z % 4) * 16 + (y % 4) * 4 + x % 4)


def greet(peers):
    barrier = pltpu.get_barrier_semaphore()
    for peer in peers:
        pl.semaphore_signal(barrier, inc=1, device_id=peer, device_id_type=pl.DeviceIdType.MESH)


def enter(peers):
    pl.semaphore_wait(pltpu.get_barrier_semaphore(), len(peers))


def gather_kernel(sc_ref, x_ref, v_ref, sx_ref, xt_ref, v_buf, lsem, ssem, rsem, tsend, trecv):
    c, z, y, x = position()
    partner = device(1 - c, z, y, x)

    def along(d):
        return device(c, z + d * (1 - c), y + d * c, x)

    peers = [partner, along(1), along(3), device(c, z, y, x + 1), device(c, z, y, x + 3)]
    x_in = pltpu.make_async_copy(x_ref, sx_ref.at[0, pl.ds(0, ROWS), :], lsem.at[0])
    v_in = pltpu.make_async_copy(v_ref, v_buf, lsem.at[1])
    x_in.start()
    v_in.start()
    greet(peers)
    x_in.wait()
    xt = jnp.transpose(sx_ref[0, 0:ROWS, :].astype(F32))
    nrm = jnp.sum(xt * xt, axis=0, keepdims=True)
    hi, mid, low = pieces(nrm)
    pos = lax.broadcasted_iota(jnp.int32, (16, 128), 0)
    one = jnp.ones((1, 128), F32)
    parts = []
    for g in range(GROUPS):
        s = slice(g * 128, (g + 1) * 128)
        parts.append((hi[:, s], mid[:, s], low[:, s]))
        xt_ref[0, g, 0:FEAT, :] = xt[:, s].astype(BF)
        xt_ref[0, g, FEAT : FEAT + 16, :] = select(pos, 0, parts[g] + (one, one, one)).astype(BF)
    enter(peers)

    copies = []

    def src_part(slot, h):
        return sx_ref.at[slot, pl.ds(h * HALF, HALF), :]

    def send(src, dst, h, dev):
        cp = pltpu.make_async_remote_copy(src_part(src, h), src_part(dst, h), ssem.at[len(copies)], rsem.at[dst, h],
                                          device_id=dev, device_id_type=pl.DeviceIdType.MESH)
        cp.start()
        copies.append(cp)

    def got(slot, h):
        pltpu.make_async_remote_copy(src_part(slot, h), src_part(slot, h), ssem.at[0], rsem.at[slot, h],
                                     device_id=partner, device_id_type=pl.DeviceIdType.MESH).wait_recv()

    tcopies = []

    def tgt_part(slot, h):
        return xt_ref.at[slot, pl.ds(h * 3, 3), pl.ds(0, XROWS), :]

    def tsnd(src, dst, h, dev):
        cp = pltpu.make_async_remote_copy(tgt_part(src, h), tgt_part(dst, h), tsend.at[len(tcopies)], trecv.at[dst, h],
                                          device_id=dev, device_id_type=pl.DeviceIdType.MESH)
        cp.start()
        tcopies.append(cp)

    def tgot(slot, h):
        pltpu.make_async_remote_copy(tgt_part(slot, h), tgt_part(slot, h), tsend.at[0], trecv.at[slot, h],
                                     device_id=partner, device_id_type=pl.DeviceIdType.MESH).wait_recv()

    right = device(c, z, y, x + 1)
    left = device(c, z, y, x + 3)
    tsnd(0, 6, 0, right)
    tsnd(0, 2, 1, left)
    tsnd(0, 6, 1, right)
    tsnd(0, 2, 0, left)
    v_in.wait()
    for g in range(GROUPS):
        sx_ref[0, ROWS + g * RHS : ROWS + (g + 1) * RHS, :] = v_buf[:, g * 128 : (g + 1) * 128]
        sx_ref[0, NBASE + g * 16 : NBASE + (g + 1) * 16, :] = select(pos, 0, (one, one, one) + parts[g]).astype(BF)
    send(0, 3, 0, along(1))
    send(0, 1, 1, along(3))
    send(0, 3, 1, along(1))
    send(0, 1, 0, along(3))
    for h in range(2):
        tsnd(0, 1, h, partner)
    for t in range(NTGT):
        for g in range(GROUPS):
            xt_ref[t, g, FEAT + 16 : 256, :] = jnp.zeros((112, 128), BF)
            if t:
                xt_ref[t, g, XROWS : FEAT + 16, :] = jnp.zeros((FEAT + 16 - XROWS, 128), BF)
    got(3, 0)
    send(3, 2, 0, along(1))
    got(1, 1)
    send(1, 2, 1, along(3))
    tgot(6, 0)
    tsnd(6, 4, 0, right)
    tgot(2, 1)
    tsnd(2, 4, 1, left)
    tsnd(6, 7, 0, partner)
    tsnd(2, 3, 1, partner)
    tgot(6, 1)
    tsnd(6, 7, 1, partner)
    tgot(2, 0)
    tsnd(2, 3, 0, partner)
    got(3, 1)
    got(1, 0)
    got(2, 0)
    got(2, 1)
    for h in range(2):
        tgot(4, h)
        tsnd(4, 5, h, partner)
    for t in (1, 3, 7, 5):
        for h in range(2):
            tgot(t, h)
    for cp in copies:
        cp.wait_send()
    for cp in tcopies:
        cp.wait_send()


def product(sc_ref, srcs, xt_ref, y_ref, tile_ref, aug_ref, eye_ref):
    alpha = jnp.concatenate([sc_ref[0:1, :], sc_ref[0:1, :]], axis=1)
    scale = jnp.concatenate([sc_ref[1:2, :], sc_ref[1:2, :]], axis=1)
    piece = 64
    n_pc = 256 // piece
    per_pair = len(srcs) * TILES
    span = 48 // per_pair
    steps = span * per_pair

    def run(*accs):
        per = 3 * n_pc + span + 1
        gram = [[[accs[q * per + r * n_pc + p] for p in range(n_pc)] for r in range(3)] for q in range(2)]
        body_acc = [[accs[q * per + 3 * n_pc + w] for q in range(2)] for w in range(span)]
        tail_acc = [accs[q * per + 3 * n_pc + span] for q in range(2)]

        def acc_gram(q, u, t, p):
            rows = pl.ds((t % TILES) * 256 + p * piece, piece)
            lhs = jnp.concatenate([srcs[t // TILES][rows, :], aug_ref[t // TILES, rows, :]], axis=1)
            pltpu.matmul_acc_lhs(gram[q][u % 3][p], lhs, load_staged_rhs=0 if p == 0 else None)

        def push_x(q, pair):
            tgt = (pair // 3) * 2 + q
            ch = (pair % 3) * 2
            pltpu.matmul_push_rhs(jnp.concatenate([xt_ref[tgt, ch], xt_ref[tgt, ch + 1]], axis=1),
                                  staging_register=0, mxu_index=q)

        def push_tile(q, u):
            pltpu.matmul_push_rhs(tile_ref[q, (u - 1) % 3], staging_register=1, mxu_index=q)

        def values(q, u, p):
            half = pltpu.matmul_pop(gram[q][(u - 2) % 3][p])
            kern = (jnp.exp2(jnp.minimum(half * alpha, 0.0)) * scale).astype(BF)
            tile_ref[q, u % 3, p * piece : (p + 1) * piece, :] = kern

        def acc_y(q, t, acc):
            lo = ROWS + (t % TILES) * 2 * RHS
            src = srcs[t // TILES]
            vt = jnp.concatenate([src[pl.ds(lo, RHS), :], src[pl.ds(lo + RHS, RHS), :]], axis=1)
            pltpu.matmul_acc_lhs(acc[q], vt, load_staged_rhs=1)

        def add_y(acc, pair):
            for q in range(2):
                y_ref[q, pair // 3, pair % 3] += pltpu.matmul_pop(acc[q])

        def clear():
            for q in range(2):
                for r in range(3):
                    for p in range(n_pc):
                        pltpu.matmul_pop(gram[q][r][p])
                for acc in body_acc:
                    pltpu.matmul_pop(acc[q])
                pltpu.matmul_pop(tail_acc[q])

        def norm_columns():
            row = lax.broadcasted_iota(jnp.int32, (256, 256), 0)
            colm = lax.broadcasted_iota(jnp.int32, (256, 256), 1)
            eye_ref[...] = jnp.where(row == colm, 1.0, 0.0).astype(BF)

            def take(n):
                for p in range(n_pc):
                    cols = pltpu.matmul_pop(gram[n % 2][(n // 2) % 3][p])
                    for h in range(2):
                        i = 2 * n + h
                        rows = pl.ds((i % TILES) * 256 + p * piece, piece)
                        aug_ref[i // TILES, rows, :] = cols[:, h * 128 : (h + 1) * 128].astype(BF)

            blank = jnp.zeros((112, 256), BF)
            count = per_pair // 2
            for n in range(count):
                rows = []
                for i in (2 * n, 2 * n + 1):
                    src = srcs[i // TILES]
                    lo = NBASE + (i % TILES) * 32
                    rows += [jnp.concatenate([src[pl.ds(lo, 16), :], src[pl.ds(lo + 16, 16), :]], axis=1), blank]
                pltpu.matmul_push_rhs(jnp.concatenate(rows, axis=0), staging_register=0, mxu_index=n % 2, transpose=True)
                for p in range(n_pc):
                    pltpu.matmul_acc_lhs(gram[n % 2][(n // 2) % 3][p], eye_ref[p * piece : (p + 1) * piece, :],
                                         load_staged_rhs=0 if p == 0 else None)
                if n >= 4:
                    take(n - 4)
            for n in range(count - 4, count):
                take(n)

        def trip(k, carry):
            old = jnp.where(k == 0, PAIRS, k * span - 1)
            for u in range(steps):
                if u < steps - 1:
                    nxt = k * span + (u + 1) // per_pair
                else:
                    nxt = jnp.minimum((k + 1) * span, PAIRS - 1)
                for q in range(2):
                    push_tile(q, u)
                for p in range(n_pc):
                    for q in range(2):
                        acc_gram(q, u, u % per_pair, p)
                        if p == 0:
                            push_x(q, nxt)
                    for q in range(2):
                        values(q, u, p)
                for q in range(2):
                    if u < 3:
                        acc_y(q, per_pair - 3 + u, tail_acc)
                    else:
                        acc_y(q, (u - 3) % per_pair, body_acc[(u - 3) // per_pair])
                if u == 1:
                    add_y(body_acc[span - 1], old)
                if u == 6:
                    add_y(tail_acc, old)
                for w in range(span - 1):
                    if u == (w + 1) * per_pair + 8:
                        add_y(body_acc[w], k * span + w)
            return carry

        clear()
        norm_columns()
        for q in range(2):
            push_x(q, 0)
        lax.fori_loop(0, PAIRS // span, trip, 0)
        for u in range(steps, steps + 3):
            for q in range(2):
                push_tile(q, u)
                if u < steps + 2:
                    for p in range(n_pc):
                        values(q, u, p)
                acc_y(q, (u - 3) % per_pair, tail_acc)
        add_y(body_acc[span - 1], PAIRS - 1)
        for q in range(2):
            acc_gram(q, 0, 0, 0)
            pltpu.matmul_pop(gram[q][0][0])
        add_y(tail_acc, PAIRS - 1)

    specs = []
    for q in range(2):
        specs += [pltpu.ACC(q)((piece, 256), F32)] * (3 * n_pc) + [pltpu.ACC(q)((RHS, 256), F32)] * (span + 1)
    pl.run_scoped(run, *specs)


def first_kernel(sc_ref, xt_ref, src_ref, y_ref, tile_ref, aug_ref, eye_ref):
    y_ref[...] = jnp.zeros_like(y_ref)
    srcs = [src_ref.at[b] for b in range(LINE)]
    product(sc_ref, srcs, xt_ref, y_ref, tile_ref, aug_ref, eye_ref)


def later_kernel(sc_ref, xt_ref, yin_ref, *refs):
    y_ref, tile_ref, aug_ref, eye_ref = refs[-4:]
    y_ref[...] = yin_ref[...]
    srcs = [ref.at[b] for ref in refs[:-4] for b in range(LINE)]
    product(sc_ref, srcs, xt_ref, y_ref, tile_ref, aug_ref, eye_ref)


def reduce_kernel(yp_ref, y_ref, part_ref, tot_ref, hop_ref, sum_ref, got_ref, psend, precv, ssem, rsem):
    c, z, y, x = position()
    partner = device(1 - c, z, y, x)
    right = device(c, z, y, x + 1)
    left = device(c, z, y, x + 3)
    peers = [partner, right, left]
    greet(peers)
    enter(peers)
    up = pl.ds(0, RHS // 2)
    down = pl.ds(RHS // 2, RHS // 2)
    copies = {}

    def send(src, dst, k, dev):
        cp = pltpu.make_async_remote_copy(src, dst, ssem.at[*k], rsem.at[*k], device_id=dev,
                                          device_id_type=pl.DeviceIdType.MESH)
        cp.start()
        copies[k] = cp

    first = {}
    for d in (2, 1, 3, 0):
        for ch in range(3):
            cp = pltpu.make_async_remote_copy(yp_ref.at[1, d, ch], part_ref.at[d, ch], psend.at[d, ch], precv.at[d, ch],
                                              device_id=partner, device_id_type=pl.DeviceIdType.MESH)
            cp.start()
            first[d, ch] = cp

    def total(d, ch):
        first[d, ch].wait()
        tot_ref[d, ch] = yp_ref[0, d, ch] + part_ref[d, ch]

    for ch in range(3):
        total(2, ch)
        send(tot_ref.at[2, ch, up, :], hop_ref.at[0, ch], (0, ch), right)
        send(tot_ref.at[2, ch, down, :], hop_ref.at[1, ch], (1, ch), left)
    for ch in range(3):
        total(1, ch)
        total(3, ch)
    for ch in range(3):
        copies[0, ch].wait_recv()
        sum_ref[0, ch] = hop_ref[0, ch] + tot_ref[1, ch, 0 : RHS // 2, :]
        send(sum_ref.at[0, ch], got_ref.at[2, ch], (4, ch), right)
        copies[1, ch].wait_recv()
        sum_ref[1, ch] = hop_ref[1, ch] + tot_ref[3, ch, RHS // 2 : RHS, :]
        send(sum_ref.at[1, ch], got_ref.at[3, ch], (5, ch), left)
        send(tot_ref.at[1, ch, down, :], got_ref.at[0, ch], (2, ch), right)
        send(tot_ref.at[3, ch, up, :], got_ref.at[1, ch], (3, ch), left)
    for ch in range(3):
        total(0, ch)
    for ch in range(3):
        for k in (2, 3, 4, 5):
            copies[k, ch].wait_recv()
        cols = slice(ch * 256, (ch + 1) * 256)
        y_ref[0 : RHS // 2, cols] = tot_ref[0, ch, 0 : RHS // 2, :] + got_ref[1, ch] + got_ref[2, ch]
        y_ref[RHS // 2 : RHS, cols] = tot_ref[0, ch, RHS // 2 : RHS, :] + got_ref[0, ch] + got_ref[3, ch]
    for cp in copies.values():
        cp.wait_send()


def cross_pairs(shift):
    pairs = []
    for c in range(2):
        for z in range(4):
            for y in range(4):
                for x in range(4):
                    z2 = (z + shift * c) % 4
                    y2 = (y + shift * (1 - c)) % 4
                    pairs.append((c * 64 + z * 16 + y * 4 + x, c * 64 + z2 * 16 + y2 * 4 + x))
    return pairs


VM = pl.BlockSpec(memory_space=pltpu.VMEM)
ANY = pl.BlockSpec(memory_space=pltpu.HBM)
FLOPS = 2 * ROWS * ROWS * (2 * FEAT + RHS) * NTGT


def solution(mesh):
    y_shape = jax.ShapeDtypeStruct((2, 5, 3, RHS, 256), F32)

    def product_call(kernel, consts, xt, args, lines):
        return pl.pallas_call(
            kernel,
            out_shape=y_shape,
            in_specs=[VM] + [VM] * (1 + len(args)),
            out_specs=VM,
            scratch_shapes=[pltpu.VMEM((2, 3, 256, 256), BF), pltpu.VMEM((lines * LINE, ROWS, 128), BF),
                            pltpu.VMEM((256, 256), BF)],
            compiler_params=pltpu.CompilerParams(vmem_limit_bytes=16 * 2**20),
            cost_estimate=pl.CostEstimate(flops=2 * FLOPS * LINE * lines, bytes_accessed=2**20, transcendentals=0),
            name="product",
        )(consts, xt, *args)

    def local_rows(x_loc, v_loc, length_scale, out_scale):
        two_ell_sq = 2.0 * length_scale[0] * length_scale[0]
        consts = jnp.broadcast_to(jnp.stack([(2.0 * LOG2E) / two_ell_sq, out_scale[0]])[:, None], (2, 128))
        line, xt = pl.pallas_call(
            gather_kernel,
            out_shape=(jax.ShapeDtypeStruct((LINE, SROWS, 128), BF), jax.ShapeDtypeStruct((NTGT, GROUPS, 256, 128), BF)),
            in_specs=[ANY, ANY, ANY],
            out_specs=(VM, VM),
            scratch_shapes=[pltpu.VMEM((RHS, ROWS), BF), pltpu.SemaphoreType.DMA((2,)),
                            pltpu.SemaphoreType.DMA((6,)), pltpu.SemaphoreType.DMA((LINE, 2)),
                            pltpu.SemaphoreType.DMA((14,)), pltpu.SemaphoreType.DMA((NTGT, 2))],
            compiler_params=pltpu.CompilerParams(collective_id=0, has_side_effects=True, vmem_limit_bytes=16 * 2**20),
            name="gather",
        )(consts, pltpu.with_memory_space_constraint(x_loc, pltpu.HBM), pltpu.with_memory_space_constraint(v_loc.T, pltpu.HBM))
        up, down = [lax.ppermute(line, ("col", "row"), cross_pairs(d)) for d in (1, 3)]
        y1 = product_call(first_kernel, consts, xt, (line,), 1)
        y1, up, down, line = lax.optimization_barrier((y1, up, down, line))
        across = lax.ppermute(line, ("col", "row"), cross_pairs(2))
        y2 = product_call(later_kernel, consts, xt, (y1, up, down), 2)
        y2, across = lax.optimization_barrier((y2, across))
        yp = product_call(later_kernel, consts, xt, (y2, across), 1)
        y_t = pl.pallas_call(
            reduce_kernel,
            out_shape=jax.ShapeDtypeStruct((RHS, ROWS), F32),
            in_specs=[VM],
            out_specs=VM,
            scratch_shapes=[pltpu.VMEM((4, 3, RHS, 256), F32), pltpu.VMEM((4, 3, RHS, 256), F32),
                            pltpu.VMEM((2, 3, RHS // 2, 256), F32), pltpu.VMEM((2, 3, RHS // 2, 256), F32),
                            pltpu.VMEM((4, 3, RHS // 2, 256), F32), pltpu.SemaphoreType.DMA((4, 3)),
                            pltpu.SemaphoreType.DMA((4, 3)), pltpu.SemaphoreType.DMA((6, 3)), pltpu.SemaphoreType.DMA((6, 3))],
            compiler_params=pltpu.CompilerParams(collective_id=1, has_side_effects=True, vmem_limit_bytes=8 * 2**20),
            name="reduce",
        )(yp)
        return y_t.T

    row_spec = P(("tasks", "row", "col"), None)
    rep_spec = P(None)
    return jax.shard_map(local_rows, mesh=mesh, in_specs=(row_spec, row_spec, rep_spec, rep_spec), out_specs=row_spec, check_vma=False)
```

```python
import functools

import jax
import jax.numpy as jnp
from jax import lax
from jax.experimental import pallas as pl
from jax.experimental.pallas import tpu as pltpu
from jax.sharding import PartitionSpec as P

BF = jnp.bfloat16
F32 = jnp.float32
ROWS = 768
FEAT = 128
RHS = 32
LINE = 4
NTGT = 8
GROUPS = 6
VROWS = GROUPS * RHS
NROWS = 8
NBASE = ROWS + VROWS
SROWS = 1024
HALF = SROWS // 2
XROWS = 136
TILES = 3
PAIRS = 12
LOG2E = 1.4426950408889634
BIG = 3.0e38


def pieces(norm):
    half = jnp.maximum(norm * -0.5, -BIG)
    hi = half.astype(BF).astype(F32)
    rest = half - hi
    mid = rest.astype(BF).astype(F32)
    return hi, mid, rest - mid


def select(pos, at, vals):
    out = jnp.zeros_like(vals[0] + pos.astype(F32))
    for k, val in enumerate(vals):
        out = jnp.where(pos == at + k, val, out)
    return out


def position():
    col = lax.axis_index("col")
    row = lax.axis_index("row")
    return col, row // 16, (row // 4) % 4, row % 4


def device(col, z, y, x):
    return (0, col, (z % 4) * 16 + (y % 4) * 4 + x % 4)


def greet(peers):
    barrier = pltpu.get_barrier_semaphore()
    for peer in peers:
        pl.semaphore_signal(barrier, inc=1, device_id=peer, device_id_type=pl.DeviceIdType.MESH)


def enter(peers):
    pl.semaphore_wait(pltpu.get_barrier_semaphore(), len(peers))


def gather_kernel(sc_ref, x_ref, v_ref, sx_ref, xt_ref, v_buf, lsem, ssem, rsem, tsend, trecv):
    c, z, y, x = position()
    partner = device(1 - c, z, y, x)

    def along(d):
        return device(c, z + d * (1 - c), y + d * c, x)

    peers = [partner, along(1), along(3), device(c, z, y, x + 1), device(c, z, y, x + 3)]
    x_in = pltpu.make_async_copy(x_ref, sx_ref.at[0, pl.ds(0, ROWS), :], lsem.at[0])
    v_in = pltpu.make_async_copy(v_ref, v_buf, lsem.at[1])
    x_in.start()
    v_in.start()
    greet(peers)
    x_in.wait()
    xt = jnp.transpose(sx_ref[0, 0:ROWS, :].astype(F32))
    nrm = jnp.sum(xt * xt, axis=0, keepdims=True)
    hi, mid, low = pieces(nrm)
    pos = lax.broadcasted_iota(jnp.int32, (16, 128), 0)
    one = jnp.ones((1, 128), F32)
    parts = []
    for g in range(GROUPS):
        s = slice(g * 128, (g + 1) * 128)
        parts.append((hi[:, s], mid[:, s], low[:, s]))
        xt_ref[0, g, 0:FEAT, :] = xt[:, s].astype(BF)
        xt_ref[0, g, FEAT : FEAT + 16, :] = select(pos, 0, parts[g] + (one, one, one)).astype(BF)
    enter(peers)

    copies = []

    def src_part(slot, h):
        return sx_ref.at[slot, pl.ds(h * HALF, HALF), :]

    def send(src, dst, h, dev):
        cp = pltpu.make_async_remote_copy(src_part(src, h), src_part(dst, h), ssem.at[len(copies)], rsem.at[dst, h],
                                          device_id=dev, device_id_type=pl.DeviceIdType.MESH)
        cp.start()
        copies.append(cp)

    def got(slot, h):
        pltpu.make_async_remote_copy(src_part(slot, h), src_part(slot, h), ssem.at[0], rsem.at[slot, h],
                                     device_id=partner, device_id_type=pl.DeviceIdType.MESH).wait_recv()

    tcopies = []

    def tgt_part(slot, h):
        return xt_ref.at[slot, pl.ds(h * 3, 3), pl.ds(0, XROWS), :]

    def tsnd(src, dst, h, dev):
        cp = pltpu.make_async_remote_copy(tgt_part(src, h), tgt_part(dst, h), tsend.at[len(tcopies)], trecv.at[dst, h],
                                          device_id=dev, device_id_type=pl.DeviceIdType.MESH)
        cp.start()
        tcopies.append(cp)

    def tgot(slot, h):
        pltpu.make_async_remote_copy(tgt_part(slot, h), tgt_part(slot, h), tsend.at[0], trecv.at[slot, h],
                                     device_id=partner, device_id_type=pl.DeviceIdType.MESH).wait_recv()

    right = device(c, z, y, x + 1)
    left = device(c, z, y, x + 3)
    tsnd(0, 6, 0, right)
    tsnd(0, 2, 1, left)
    tsnd(0, 6, 1, right)
    tsnd(0, 2, 0, left)
    v_in.wait()
    for g in range(GROUPS):
        sx_ref[0, ROWS + g * RHS : ROWS + (g + 1) * RHS, :] = v_buf[:, g * 128 : (g + 1) * 128]
        sx_ref[0, NBASE + g * NROWS : NBASE + g * NROWS + 16, :] = select(pos, 0, (one, one, one) + parts[g]).astype(BF)
    sx_ref[0, SROWS - 8 : SROWS, :] = jnp.zeros((8, 128), BF)
    send(0, 3, 0, along(1))
    send(0, 1, 1, along(3))
    send(0, 3, 1, along(1))
    send(0, 1, 0, along(3))
    for h in range(2):
        tsnd(0, 1, h, partner)
    for t in range(NTGT):
        for g in range(GROUPS):
            xt_ref[t, g, FEAT + 16 : 256, :] = jnp.zeros((112, 128), BF)
            if t:
                xt_ref[t, g, XROWS : FEAT + 16, :] = jnp.zeros((FEAT + 16 - XROWS, 128), BF)
    got(3, 0)
    send(3, 2, 0, along(1))
    got(1, 1)
    send(1, 2, 1, along(3))
    tgot(6, 0)
    tsnd(6, 4, 0, right)
    tgot(2, 1)
    tsnd(2, 4, 1, left)
    tsnd(6, 7, 0, partner)
    tsnd(2, 3, 1, partner)
    tgot(6, 1)
    tsnd(6, 7, 1, partner)
    tgot(2, 0)
    tsnd(2, 3, 0, partner)
    got(3, 1)
    got(1, 0)
    got(2, 0)
    got(2, 1)
    for h in range(2):
        tgot(4, h)
        tsnd(4, 5, h, partner)
    for t in (1, 3, 7, 5):
        for h in range(2):
            tgot(t, h)
    for cp in copies:
        cp.wait_send()
    for cp in tcopies:
        cp.wait_send()


def product(sc_ref, srcs, xt_ref, y_ref, tile_ref, aug_ref, eye_ref):
    alpha = jnp.concatenate([sc_ref[0:1, :], sc_ref[0:1, :]], axis=1)
    scale = jnp.concatenate([sc_ref[1:2, :], sc_ref[1:2, :]], axis=1)
    piece = 64
    n_pc = 256 // piece
    per_pair = len(srcs) * TILES
    span = 48 // per_pair
    steps = span * per_pair

    def run(*accs):
        per = 3 * n_pc + span + 1
        gram = [[[accs[q * per + r * n_pc + p] for p in range(n_pc)] for r in range(3)] for q in range(2)]
        body_acc = [[accs[q * per + 3 * n_pc + w] for q in range(2)] for w in range(span)]
        tail_acc = [accs[q * per + 3 * n_pc + span] for q in range(2)]

        def acc_gram(q, u, t, p):
            rows = pl.ds((t % TILES) * 256 + p * piece, piece)
            lhs = jnp.concatenate([srcs[t // TILES][rows, :], aug_ref[t // TILES, rows, :]], axis=1)
            pltpu.matmul_acc_lhs(gram[q][u % 3][p], lhs, load_staged_rhs=0 if p == 0 else None)

        def push_x(q, pair):
            tgt = (pair // 3) * 2 + q
            ch = (pair % 3) * 2
            pltpu.matmul_push_rhs(jnp.concatenate([xt_ref[tgt, ch], xt_ref[tgt, ch + 1]], axis=1),
                                  staging_register=0, mxu_index=q)

        def push_tile(q, u):
            pltpu.matmul_push_rhs(tile_ref[q, (u - 1) % 3], staging_register=1, mxu_index=q)

        def values(q, u, p):
            half = pltpu.matmul_pop(gram[q][(u - 2) % 3][p])
            kern = (jnp.exp2(jnp.minimum(half * alpha, 0.0)) * scale).astype(BF)
            tile_ref[q, u % 3, p * piece : (p + 1) * piece, :] = kern

        def acc_y(q, t, acc):
            lo = ROWS + (t % TILES) * 2 * RHS
            src = srcs[t // TILES]
            vt = jnp.concatenate([src[pl.ds(lo, RHS), :], src[pl.ds(lo + RHS, RHS), :]], axis=1)
            pltpu.matmul_acc_lhs(acc[q], vt, load_staged_rhs=1)

        def add_y(acc, pair):
            for q in range(2):
                y_ref[q, pair // 3, pair % 3] += pltpu.matmul_pop(acc[q])

        def clear():
            for q in range(2):
                for r in range(3):
                    for p in range(n_pc):
                        pltpu.matmul_pop(gram[q][r][p])
                for acc in body_acc:
                    pltpu.matmul_pop(acc[q])
                pltpu.matmul_pop(tail_acc[q])

        def norm_columns():
            row = lax.broadcasted_iota(jnp.int32, (256, 256), 0)
            colm = lax.broadcasted_iota(jnp.int32, (256, 256), 1)
            eye_ref[...] = jnp.where(row == colm, 1.0, 0.0).astype(BF)

            def take(n):
                for p in range(n_pc):
                    cols = pltpu.matmul_pop(gram[n % 2][(n // 2) % 3][p])
                    for h in range(2):
                        i = 2 * n + h
                        rows = pl.ds((i % TILES) * 256 + p * piece, piece)
                        aug_ref[i // TILES, rows, :] = cols[:, h * 128 : (h + 1) * 128].astype(BF)

            blank = jnp.zeros((112, 256), BF)
            count = per_pair // 2
            for n in range(count):
                rows = []
                for i in (2 * n, 2 * n + 1):
                    src = srcs[i // TILES]
                    lo = NBASE + (i % TILES) * 2 * NROWS
                    rows += [jnp.concatenate([src[pl.ds(lo, 16), :], src[pl.ds(lo + NROWS, 16), :]], axis=1), blank]
                pltpu.matmul_push_rhs(jnp.concatenate(rows, axis=0), staging_register=0, mxu_index=n % 2, transpose=True)
                for p in range(n_pc):
                    pltpu.matmul_acc_lhs(gram[n % 2][(n // 2) % 3][p], eye_ref[p * piece : (p + 1) * piece, :],
                                         load_staged_rhs=0 if p == 0 else None)
                if n >= 4:
                    take(n - 4)
            for n in range(count - 4, count):
                take(n)

        def trip(k, carry):
            old = jnp.where(k == 0, PAIRS, k * span - 1)
            for u in range(steps):
                if u < steps - 1:
                    nxt = k * span + (u + 1) // per_pair
                else:
                    nxt = jnp.minimum((k + 1) * span, PAIRS - 1)
                for q in range(2):
                    push_tile(q, u)
                for p in range(n_pc):
                    for q in range(2):
                        acc_gram(q, u, u % per_pair, p)
                        if p == 0:
                            push_x(q, nxt)
                    for q in range(2):
                        values(q, u, p)
                for q in range(2):
                    if u < 3:
                        acc_y(q, per_pair - 3 + u, tail_acc)
                    else:
                        acc_y(q, (u - 3) % per_pair, body_acc[(u - 3) // per_pair])
                if u == 1:
                    add_y(body_acc[span - 1], old)
                if u == 6:
                    add_y(tail_acc, old)
                for w in range(span - 1):
                    if u == (w + 1) * per_pair + 8:
                        add_y(body_acc[w], k * span + w)
            return carry

        clear()
        norm_columns()
        for q in range(2):
            push_x(q, 0)
        lax.fori_loop(0, PAIRS // span, trip, 0)
        for u in range(steps, steps + 3):
            for q in range(2):
                push_tile(q, u)
                if u < steps + 2:
                    for p in range(n_pc):
                        values(q, u, p)
                acc_y(q, (u - 3) % per_pair, tail_acc)
        add_y(body_acc[span - 1], PAIRS - 1)
        for q in range(2):
            acc_gram(q, 0, 0, 0)
            pltpu.matmul_pop(gram[q][0][0])
        add_y(tail_acc, PAIRS - 1)

    specs = []
    for q in range(2):
        specs += [pltpu.ACC(q)((piece, 256), F32)] * (3 * n_pc) + [pltpu.ACC(q)((RHS, 256), F32)] * (span + 1)
    pl.run_scoped(run, *specs)


def first_kernel(sc_ref, xt_ref, src_ref, y_ref, tile_ref, aug_ref, eye_ref):
    y_ref[...] = jnp.zeros_like(y_ref)
    srcs = [src_ref.at[b] for b in range(LINE)]
    product(sc_ref, srcs, xt_ref, y_ref, tile_ref, aug_ref, eye_ref)


def later_kernel(sc_ref, xt_ref, yin_ref, *refs):
    y_ref, tile_ref, aug_ref, eye_ref = refs[-4:]
    y_ref[...] = yin_ref[...]
    srcs = [ref.at[b] for ref in refs[:-4] for b in range(LINE)]
    product(sc_ref, srcs, xt_ref, y_ref, tile_ref, aug_ref, eye_ref)


def reduce_kernel(yp_ref, y_ref, part_ref, tot_ref, hop_ref, sum_ref, got_ref, psend, precv, ssem, rsem):
    c, z, y, x = position()
    partner = device(1 - c, z, y, x)
    right = device(c, z, y, x + 1)
    left = device(c, z, y, x + 3)
    peers = [partner, right, left]
    greet(peers)
    enter(peers)
    up = pl.ds(0, RHS // 2)
    down = pl.ds(RHS // 2, RHS // 2)
    copies = []

    def send(src, dst, k, dev):
        cp = pltpu.make_async_remote_copy(src, dst, ssem.at[k], rsem.at[k], device_id=dev,
                                          device_id_type=pl.DeviceIdType.MESH)
        cp.start()
        copies.append(cp)

    first = {}
    for d in (2, 1, 3, 0):
        first[d] = pltpu.make_async_remote_copy(yp_ref.at[1, d], part_ref.at[d], psend.at[d], precv.at[d],
                                                device_id=partner, device_id_type=pl.DeviceIdType.MESH)
        first[d].start()

    def total(d):
        first[d].wait()
        tot_ref[d] = yp_ref[0, d] + part_ref[d]

    total(2)
    send(tot_ref.at[2, :, up, :], hop_ref.at[0], 0, right)
    send(tot_ref.at[2, :, down, :], hop_ref.at[1], 1, left)
    total(1)
    send(tot_ref.at[1, :, down, :], got_ref.at[0], 2, right)
    total(3)
    send(tot_ref.at[3, :, up, :], got_ref.at[1], 3, left)
    total(0)
    copies[0].wait_recv()
    sum_ref[0] = hop_ref[0] + tot_ref[1, :, 0 : RHS // 2, :]
    send(sum_ref.at[0], got_ref.at[2], 4, right)
    copies[1].wait_recv()
    sum_ref[1] = hop_ref[1] + tot_ref[3, :, RHS // 2 : RHS, :]
    send(sum_ref.at[1], got_ref.at[3], 5, left)
    for k in (2, 3, 4, 5):
        copies[k].wait_recv()
    for ch in range(3):
        cols = slice(ch * 256, (ch + 1) * 256)
        y_ref[0 : RHS // 2, cols] = tot_ref[0, ch, 0 : RHS // 2, :] + got_ref[1, ch] + got_ref[2, ch]
        y_ref[RHS // 2 : RHS, cols] = tot_ref[0, ch, RHS // 2 : RHS, :] + got_ref[0, ch] + got_ref[3, ch]
    for cp in copies:
        cp.wait_send()


def cross_pairs(shift):
    pairs = []
    for c in range(2):
        for z in range(4):
            for y in range(4):
                for x in range(4):
                    z2 = (z + shift * c) % 4
                    y2 = (y + shift * (1 - c)) % 4
                    pairs.append((c * 64 + z * 16 + y * 4 + x, c * 64 + z2 * 16 + y2 * 4 + x))
    return pairs


VM = pl.BlockSpec(memory_space=pltpu.VMEM)
ANY = pl.BlockSpec(memory_space=pltpu.HBM)
FLOPS = 2 * ROWS * ROWS * (2 * FEAT + RHS) * NTGT


def solution(mesh):
    y_shape = jax.ShapeDtypeStruct((2, 5, 3, RHS, 256), F32)

    def product_call(kernel, consts, xt, args, lines):
        return pl.pallas_call(
            kernel,
            out_shape=y_shape,
            in_specs=[VM] + [VM] * (1 + len(args)),
            out_specs=VM,
            scratch_shapes=[pltpu.VMEM((2, 3, 256, 256), BF), pltpu.VMEM((lines * LINE, ROWS, 128), BF),
                            pltpu.VMEM((256, 256), BF)],
            compiler_params=pltpu.CompilerParams(vmem_limit_bytes=16 * 2**20),
            cost_estimate=pl.CostEstimate(flops=2 * FLOPS * LINE * lines, bytes_accessed=2**20, transcendentals=0),
            name="product",
        )(consts, xt, *args)

    def local_rows(x_loc, v_loc, length_scale, out_scale):
        two_ell_sq = 2.0 * length_scale[0] * length_scale[0]
        consts = jnp.broadcast_to(jnp.stack([(2.0 * LOG2E) / two_ell_sq, out_scale[0]])[:, None], (2, 128))
        line, xt = pl.pallas_call(
            gather_kernel,
            out_shape=(jax.ShapeDtypeStruct((LINE, SROWS, 128), BF), jax.ShapeDtypeStruct((NTGT, GROUPS, 256, 128), BF)),
            in_specs=[ANY, ANY, ANY],
            out_specs=(VM, VM),
            scratch_shapes=[pltpu.VMEM((RHS, ROWS), BF), pltpu.SemaphoreType.DMA((2,)),
                            pltpu.SemaphoreType.DMA((6,)), pltpu.SemaphoreType.DMA((LINE, 2)),
                            pltpu.SemaphoreType.DMA((14,)), pltpu.SemaphoreType.DMA((NTGT, 2))],
            compiler_params=pltpu.CompilerParams(collective_id=0, has_side_effects=True, vmem_limit_bytes=16 * 2**20),
            name="gather",
        )(consts, pltpu.with_memory_space_constraint(x_loc, pltpu.HBM), pltpu.with_memory_space_constraint(v_loc.T, pltpu.HBM))
        up, down = [lax.ppermute(line, ("col", "row"), cross_pairs(d)) for d in (1, 3)]
        y1 = product_call(first_kernel, consts, xt, (line,), 1)
        y1, up, down, line = lax.optimization_barrier((y1, up, down, line))
        across = lax.ppermute(line, ("col", "row"), cross_pairs(2))
        y2 = product_call(later_kernel, consts, xt, (y1, up, down), 2)
        y2, across = lax.optimization_barrier((y2, across))
        yp = product_call(later_kernel, consts, xt, (y2, across), 1)
        y_t = pl.pallas_call(
            reduce_kernel,
            out_shape=jax.ShapeDtypeStruct((RHS, ROWS), F32),
            in_specs=[VM],
            out_specs=VM,
            scratch_shapes=[pltpu.VMEM((4, 3, RHS, 256), F32), pltpu.VMEM((4, 3, RHS, 256), F32),
                            pltpu.VMEM((2, 3, RHS // 2, 256), F32), pltpu.VMEM((2, 3, RHS // 2, 256), F32),
                            pltpu.VMEM((4, 3, RHS // 2, 256), F32), pltpu.SemaphoreType.DMA((4,)),
                            pltpu.SemaphoreType.DMA((4,)), pltpu.SemaphoreType.DMA((6,)), pltpu.SemaphoreType.DMA((6,))],
            compiler_params=pltpu.CompilerParams(collective_id=1, has_side_effects=True, vmem_limit_bytes=8 * 2**20),
            name="reduce",
        )(yp)
        return y_t.T

    row_spec = P(("tasks", "row", "col"), None)
    rep_spec = P(None)
    return jax.shard_map(local_rows, mesh=mesh, in_specs=(row_spec, row_spec, rep_spec, rep_spec), out_specs=row_spec, check_vma=False)
```
